256 devices in a mesh: seq: 32 (over y, x, core), head: 8 (over z).
Axes of the slice: x: 4, y: 4, z: 8, core: 2. Of those that a mesh axis runs over, the one named last changes fastest.
Arguments:
- tokens: bfloat16 [512, 4096], P('seq'), may hold values from -6 to 6
- norm_gain: bfloat16 [4096], replicated, may hold values from 0.25 to 1.75
- w_query: bfloat16 [4096, 4096], P(None, 'head'), may hold values from -0.09375 to 0.09375
- key_projection: bfloat16 [4096, 1024], P(None, 'head'), may hold values from -0.25 to 0.25
- value_projection: bfloat16 [4096, 1024], P(None, 'head'), may hold values from -0.09375 to 0.09375
- w_out: bfloat16 [4096, 4096], P('head'), may hold values from -0.09375 to 0.09375
- cache_keys: bfloat16 [8, 65536, 1024], P(None, 'seq', 'head'), may hold values from -60 to 60
- paged_value_cache: bfloat16 [8, 65536, 1024], P(None, 'seq', 'head'), may hold values from -6 to 6
- lengths: int32 [8], replicated, may hold values from 8192 to 65536
- parents: int32 [8, 64], replicated, may hold values from -1 to 62, as said below
- slot_block: int32 [8, 512], P(None, 'seq'), may hold values from 0 to 511, each once within a row
Outputs:
- mixed: bfloat16 [512, 4096], P('seq', 'head')
The draws below stay inside these ranges and needn't reach their ends.
Inputs may be any that keep to these rules, and one draw needn't show every extreme that they name: parents[r, 0] = -1 for the root; for j >= 1, 0 <= parents[r, j] < j; the last token's parent is always token 62. Each row of slot_block is a permutation of 0 to 511.
All inputs are finite; a program needn't handle non-finite values.
Results may differ from the reference program's by a relative error of at most 0.0054.
The reference program's roundings to bfloat16 on the way count: a program that leaves them out, or rounds other values in their place, can miss the bound.
Values may be sent and summed in bfloat16 or wider, within the bound.
A program may use at most 128 MiB of HBM per device.

```python
import jax
import jax.numpy as jnp
from jax import lax

MODEL_WIDTH = 4096
HQ = 32
KEY_VALUE_HEADS = 8
HEAD_WIDTH = 128
TQ = 64
BLK = 128
REQUEST_COUNT = 8
CTX_DEV = 2048
CONTEXT_SLOTS = 65536
NBLK = 512
TOKENS = 512
N_SEQ = 32


def draw_parents(key, part):
    node_ids = jnp.arange(TQ, dtype=jnp.int32)
    raw_bits = jax.random.randint(key, (REQUEST_COUNT, TQ), 0, 1 << 20, dtype=jnp.int32)
    picked = raw_bits % jnp.maximum(node_ids, 1)[None, :]
    picked = jnp.where(node_ids[None, :] == TQ - 1, TQ - 2, picked)
    picked = jnp.where(node_ids[None, :] == 0, -1, picked)
    return picked.astype(jnp.int32)


def draw_cache_keys(key, part):
    complete_shape = (REQUEST_COUNT, CONTEXT_SLOTS, KEY_VALUE_HEADS * HEAD_WIDTH)
    drawn = 3.0 * jax.random.truncated_normal(key, -5.0, 5.0, complete_shape, jnp.float32)
    return drawn.astype(jnp.bfloat16)


def with_ends(array, rng, low, top_value):
    dims = array.shape
    index_at = [jax.random.randint(jax.random.fold_in(rng, axis), (), 0, dims[axis]) for axis in range(len(dims))]
    array = array.at[tuple(index_at)].set(low)
    longest = dims.index(max(dims))
    index_at[longest] = (index_at[longest] + 1) % dims[longest]
    return array.at[tuple(index_at)].set(top_value)


def steps_of(rng, extent, shards, least, high):
    loudness, own = 1.0, jax.random.fold_in(rng, 6)
    for dim, parts in shards:
        heights = jnp.exp(jax.random.uniform(jax.random.fold_in(own, dim), (parts,), jnp.float32, least / len(shards), high / len(shards)))
        loudness = loudness * jnp.repeat(heights, extent[dim] // parts).reshape([-1 if axis == dim else 1 for axis in range(len(extent))])
    return loudness


def noise(rng, dims, width, reach, cuts=(), held_as=jnp.bfloat16):
    entries = jax.random.normal(rng, dims, jnp.float32) * width
    if len(cuts) > 0:
        entries = steps_of(rng, dims, cuts, -0.22, 0.18) * entries
    return jnp.clip(entries, min=-reach, max=reach).astype(held_as)


def setup_inputs(seed: int = 0) -> dict:
    seeds = jax.random.split(jax.random.key(seed), 12)
    return {
        "tokens": noise(seeds[0], (TOKENS, MODEL_WIDTH), 1.0, 6.0, ((0, 32),)),
        "norm_gain": jnp.clip(1.0 + 0.15 * jax.random.normal(seeds[1], (MODEL_WIDTH,), jnp.float32), 0.25, 1.75).astype(jnp.bfloat16),
        "w_query": noise(seeds[2], (MODEL_WIDTH, HQ * HEAD_WIDTH), MODEL_WIDTH ** -0.5, 0.09375, ((1, 8),)),
        "key_projection": noise(seeds[3], (MODEL_WIDTH, KEY_VALUE_HEADS * HEAD_WIDTH), (MODEL_WIDTH // 9) ** -0.5, 0.25, ((1, 8),)),
        "value_projection": noise(seeds[4], (MODEL_WIDTH, KEY_VALUE_HEADS * HEAD_WIDTH), MODEL_WIDTH ** -0.5, 0.09375, ((1, 8),)),
        "w_out": noise(seeds[5], (HQ * HEAD_WIDTH, MODEL_WIDTH), (HQ * HEAD_WIDTH) ** -0.5, 0.09375, ((0, 8),)),
        "cache_keys": draw_cache_keys(jax.random.fold_in(seeds[11], 71), 0),
        "paged_value_cache": noise(seeds[7], (REQUEST_COUNT, CONTEXT_SLOTS, KEY_VALUE_HEADS * HEAD_WIDTH), 1.0, 6.0, ((1, 32), (2, 8))),
        "lengths": with_ends(jax.random.randint(seeds[8], (REQUEST_COUNT,), CONTEXT_SLOTS // 8, CONTEXT_SLOTS + 1), jax.random.fold_in(seeds[8], 1), CONTEXT_SLOTS // 8, CONTEXT_SLOTS).astype(jnp.int32),
        "parents": draw_parents(jax.random.fold_in(seeds[11], 71), 0),
        "slot_block": jax.vmap(lambda own: jax.random.permutation(own, NBLK))(jax.random.split(seeds[10], REQUEST_COUNT)).reshape((REQUEST_COUNT, NBLK)).astype(jnp.int32),
    }


norm_epsilon = 1e-05
masked_score = -1e+30

def ancestors(parents):
    width_tree = parents.shape[-1]
    node_ids = jnp.arange(width_tree, dtype=jnp.int32)
    reached = (parents[..., :, None] == node_ids).astype(jnp.float32)
    reached = reached + (node_ids[:, None] == node_ids[None, :]).astype(jnp.float32)
    for repeat_step in range(max(1, (width_tree - 1).bit_length())):
        reached = jnp.minimum(jnp.einsum('rij,rjk->rik', reached, reached, precision=lax.Precision.HIGHEST), 1.0)
    return reached

def finish_group(group_max, group_total, group_sum):
    floored = jnp.maximum(group_total, 1.0)
    output = lax.optimization_barrier((group_sum / floored[..., None]).astype(jnp.bfloat16)).astype(jnp.float32)
    return (output, group_max + jnp.log(floored))

def reference(tokens, norm_gain, w_query, key_projection, value_projection, w_out, cache_keys, paged_value_cache, lengths, parents, slot_block):
    inputs = tokens.astype(jnp.float32)
    normed = (inputs * lax.rsqrt(lax.optimization_barrier(jnp.mean(inputs * inputs, axis=-1, keepdims=True)) + norm_epsilon) * norm_gain.astype(jnp.float32)).astype(jnp.bfloat16)
    queries = jnp.dot(normed, w_query, preferred_element_type=jnp.float32).astype(jnp.bfloat16)
    key_new = jnp.dot(normed, key_projection, preferred_element_type=jnp.float32).astype(jnp.bfloat16)
    value_new = jnp.dot(normed, value_projection, preferred_element_type=jnp.float32).astype(jnp.bfloat16)
    kv_heads = key_projection.shape[1] // HEAD_WIDTH
    groups = w_query.shape[1] // key_projection.shape[1]
    context = cache_keys.shape[1]
    requests = lengths.shape[0]
    score_scale = HEAD_WIDTH ** (-0.5)
    tree_mask = ancestors(parents) > 0.5
    block_offsets = jnp.arange(BLK, dtype=jnp.int32)
    positions = (slot_block[:, :, None] * BLK + block_offsets[None, None, :]).reshape(requests, context)
    visible = positions < lengths[:, None]

    def one_request(packed):
        query_rows, key_rows, value_rows, key_tree, value_tree, seen, tree_seen = packed
        query32 = query_rows.astype(jnp.float32)
        key32 = key_rows.astype(jnp.float32).reshape(N_SEQ, CTX_DEV, kv_heads, HEAD_WIDTH)
        value32 = value_rows.astype(jnp.float32).reshape(N_SEQ, CTX_DEV, kv_heads, HEAD_WIDTH)
        scores = jnp.einsum('thgd,nchd->thgnc', query32, key32, precision=lax.Precision.HIGHEST) * score_scale
        seen_groups = seen.reshape(N_SEQ, CTX_DEV)
        scores = jnp.where(seen_groups, scores, masked_score)
        group_max = scores.max(-1)
        weights = jnp.where(seen_groups, jnp.exp(scores - group_max[..., None]), 0.0)
        group_total = weights.sum(-1)
        rounded = lax.optimization_barrier(weights.astype(jnp.bfloat16)).astype(jnp.float32)
        group_sum = jnp.einsum('thgnc,nchd->thgnd', rounded, value32, precision=lax.Precision.HIGHEST)
        group_out, group_lse = finish_group(group_max, group_total, group_sum)
        tree_scores = jnp.einsum('thgd,uhd->thgu', query32, key_tree.astype(jnp.float32), precision=lax.Precision.HIGHEST) * score_scale
        tree_visible = tree_seen[:, None, None, :]
        tree_scores = jnp.where(tree_visible, tree_scores, masked_score)
        tree_max = tree_scores.max(-1)
        tree_weights = jnp.where(tree_visible, jnp.exp(tree_scores - tree_max[..., None]), 0.0)
        tree_total = tree_weights.sum(-1)
        tree_rounded = lax.optimization_barrier(tree_weights.astype(jnp.bfloat16)).astype(jnp.float32)
        tree_sum = jnp.einsum('thgu,uhd->thgd', tree_rounded, value_tree.astype(jnp.float32), precision=lax.Precision.HIGHEST)
        tree_out, tree_lse = finish_group(tree_max, tree_total, tree_sum)
        best = jnp.maximum(group_lse.max(-1), tree_lse)
        group_factor = jnp.exp(group_lse - best[..., None])
        tree_factor = jnp.exp(tree_lse - best)
        numerator = (group_out * group_factor[..., None]).sum(-2) + tree_out * tree_factor[..., None]
        total = group_factor.sum(-1) + tree_factor
        attended = (numerator / total[..., None]).astype(jnp.bfloat16)
        return attended.reshape(attended.shape[0], -1)
    packed = (queries.reshape(requests, TQ, kv_heads, groups, HEAD_WIDTH), cache_keys, paged_value_cache, key_new.reshape(requests, TQ, kv_heads, HEAD_WIDTH), value_new.reshape(requests, TQ, kv_heads, HEAD_WIDTH), visible, tree_mask)
    attended = lax.map(one_request, packed).reshape(requests * TQ, -1)
    mixed = inputs + jnp.dot(attended, w_out, preferred_element_type=jnp.float32)
    return mixed.astype(jnp.bfloat16)
```

```python
import functools
import math

import jax
import jax.numpy as jnp
from jax import lax
from jax.experimental import pallas as pl
from jax.experimental.pallas import tpu as pltpu
from jax.sharding import PartitionSpec as P

NORM_EPSILON = 1e-05
HIDDEN = -1e30
HEAD_WIDTH = 128
TREE = 64
PAGE = 128
KEY_TILE = 256
WEIGHT_PARTS = 4

NT = (((1,), (1,)), ((), ()))
TN = (((0,), (0,)), ((), ()))
F32 = jnp.float32
BF16 = jnp.bfloat16


def layer(
    n_seq,
    n_head,
    lengths_ref,
    slots_ref,
    tokens_ref,
    gain_ref,
    parents_ref,
    wq_hbm,
    wk_hbm,
    wv_hbm,
    wo_hbm,
    keys_hbm,
    values_hbm,
    mixed_ref,
    wqkv,
    wo,
    keys,
    values,
    normed,
    qall,
    kvtree,
    score_a,
    score_b,
    top_a,
    top_b,
    out_send,
    lse_send,
    out_recv,
    lse_recv,
    part_send,
    part_recv,
    w_sem,
    wo_sem,
    k_sem,
    v_sem,
    q_send_sem,
    q_recv_sem,
    kv_send_sem,
    kv_recv_sem,
    o_send_sem,
    o_recv_sem,
    l_send_sem,
    l_recv_sem,
    p_send_sem,
    p_recv_sem,
):
    me = lax.axis_index("seq")
    head = lax.axis_index("head")
    rows, width = tokens_ref.shape
    requests = keys.shape[0]
    context = keys.shape[1]
    owners = TREE // rows
    q_width = wq_hbm.shape[1]
    groups = q_width // HEAD_WIDTH
    block = groups * rows
    queries = owners * block
    tiles = context // KEY_TILE
    own_request = me // owners
    own_place = me % owners
    scale = HEAD_WIDTH**-0.5
    scale2 = scale * math.log2(math.e)

    part = width // WEIGHT_PARTS

    def weight_copies(c):
        at = pl.ds(c * part, part)
        return (
            pltpu.make_async_copy(
                wq_hbm.at[at], wqkv.at[at, pl.ds(0, q_width)], w_sem.at[0, c]
            ),
            pltpu.make_async_copy(
                wk_hbm.at[at], wqkv.at[at, pl.ds(q_width, HEAD_WIDTH)], w_sem.at[1, c]
            ),
            pltpu.make_async_copy(
                wv_hbm.at[at],
                wqkv.at[at, pl.ds(q_width + HEAD_WIDTH, HEAD_WIDTH)],
                w_sem.at[2, c],
            ),
        )

    def key_copy(r):
        return pltpu.make_async_copy(keys_hbm.at[r], keys.at[r], k_sem.at[r])

    def value_copy(r):
        return pltpu.make_async_copy(values_hbm.at[r], values.at[r], v_sem.at[r])

    own_width = width // n_head

    def wo_copy(j):
        at = pl.ds(pl.multiple_of(j * own_width, own_width), own_width)
        return pltpu.make_async_copy(wo_hbm.at[:, at], wo.at[j], wo_sem.at[j])

    def request_at(i):
        return (own_request + i) % requests

    for c in range(WEIGHT_PARTS):
        for copy in weight_copies(c):
            copy.start()

    def start_cache(i, _):
        key_copy(request_at(i)).start()
        value_copy(request_at(i)).start()
        return 0

    lax.fori_loop(1, requests + 1, start_cache, 0)

    def start_wo(j, _):
        wo_copy(j).start()
        return 0

    lax.fori_loop(0, n_head, start_wo, 0)

    barrier = pltpu.get_barrier_semaphore()

    def greet_seq(j, _):
        pl.semaphore_signal(
            barrier,
            inc=1,
            device_id=((me + j) % n_seq, head),
            device_id_type=pl.DeviceIdType.MESH,
        )
        return 0

    def greet_head(j, _):
        pl.semaphore_signal(
            barrier,
            inc=1,
            device_id=(me, (head + j) % n_head),
            device_id_type=pl.DeviceIdType.MESH,
        )
        return 0

    lax.fori_loop(1, n_seq, greet_seq, 0)
    lax.fori_loop(1, n_head, greet_head, 0)

    inputs = tokens_ref[...].astype(F32)
    mean = jnp.mean(inputs * inputs, axis=-1, keepdims=True)
    normed[...] = (
        inputs * lax.rsqrt(mean + NORM_EPSILON) * gain_ref[...].astype(F32)
    ).astype(BF16)

    parent = parents_ref[pl.ds(own_request, 1), :]
    node = lax.broadcasted_iota(jnp.int32, (TREE, TREE), 0)
    other = lax.broadcasted_iota(jnp.int32, (TREE, TREE), 1)
    reached = jnp.where((parent == node) | (node == other), 1.0, 0.0)
    for _ in range(max(1, (TREE - 1).bit_length())):
        half = reached.astype(BF16)
        reached = jnp.minimum(jnp.dot(half, half, preferred_element_type=F32), 1.0)

    projected = jnp.zeros((rows, wqkv.shape[1]), F32)
    for c in range(WEIGHT_PARTS):
        for copy in weight_copies(c):
            copy.wait()
        projected += jnp.dot(
            normed[:, c * part : (c + 1) * part],
            wqkv[c * part : (c + 1) * part, :],
            preferred_element_type=F32,
        )
    projected = projected.astype(BF16)
    for g in range(groups):
        qall[me, g * rows : (g + 1) * rows, :] = projected[
            :, g * HEAD_WIDTH : (g + 1) * HEAD_WIDTH
        ]
    for n in range(2):
        kvtree[own_place, n * rows : (n + 1) * rows, :] = projected[
            :, q_width + n * HEAD_WIDTH : q_width + (n + 1) * HEAD_WIDTH
        ]

    def q_copy(peer):
        return pltpu.make_async_remote_copy(
            src_ref=qall.at[me],
            dst_ref=qall.at[me],
            send_sem=q_send_sem,
            recv_sem=q_recv_sem.at[own_request],
            device_id=(peer, head),
            device_id_type=pl.DeviceIdType.MESH,
        )

    pl.semaphore_wait(barrier, n_seq - 1 + n_head - 1)

    def kv_send(j, _):
        peer = own_request * owners + (own_place + j) % owners
        pltpu.make_async_remote_copy(
            src_ref=kvtree.at[own_place],
            dst_ref=kvtree.at[own_place],
            send_sem=kv_send_sem,
            recv_sem=kv_recv_sem,
            device_id=(peer, head),
            device_id_type=pl.DeviceIdType.MESH,
        ).start()
        return 0

    def q_send(n, _):
        to = (own_request + requests - 1 - n // owners) % requests
        q_copy(to * owners + (own_place + n) % owners).start()
        return 0

    def q_send_own(j, _):
        q_copy(own_request * owners + (own_place + j) % owners).start()
        return 0

    lax.fori_loop(0, owners, q_send, 0)
    lax.fori_loop(1, owners, kv_send, 0)
    lax.fori_loop(owners, (requests - 1) * owners, q_send, 0)
    lax.fori_loop(1, owners, q_send_own, 0)

    pltpu.make_async_copy(
        kvtree.at[pl.ds(0, owners - 1)], kvtree.at[pl.ds(0, owners - 1)], kv_recv_sem
    ).wait()
    lanes = 128
    own_queries = qall[me]
    own_queries = jnp.concatenate([own_queries] * (lanes // block), axis=0)
    tree_keys = kvtree[:, :rows, :].reshape(TREE, HEAD_WIDTH)
    tree_values = kvtree[:, rows:, :].reshape(TREE, HEAD_WIDTH)
    token = lax.broadcasted_iota(jnp.int32, (TREE, lanes), 0)
    lane = lax.broadcasted_iota(jnp.int32, (TREE, lanes), 1)
    pick = jnp.where(token == own_place * rows + lane % rows, 1.0, 0.0).astype(BF16)
    seen = jnp.dot(reached.astype(BF16), pick, preferred_element_type=F32) > 0.5
    tree_scores = lax.dot_general(
        tree_keys, own_queries, NT, preferred_element_type=F32
    )
    tree_scores = jnp.where(seen, tree_scores, HIDDEN)
    tree_top = jnp.max(tree_scores, axis=0, keepdims=True)
    tree_weights = jnp.where(
        seen, jnp.exp2(tree_scores * scale2 - tree_top * scale2), 0.0
    )
    tree_total = jnp.maximum(jnp.sum(tree_weights, axis=0, keepdims=True), 1.0)
    tree_sum = lax.dot_general(
        tree_values, tree_weights.astype(BF16), TN, preferred_element_type=F32
    )
    tree_out = (tree_sum / tree_total).astype(BF16).astype(F32).T[:block]
    tree_lse = tree_top * scale + jnp.log(tree_total)

    row_in_page = lax.broadcasted_iota(jnp.int32, (PAGE, queries), 0)

    def wait_for(i):
        r = request_at(i)

        @pl.when(i < requests)
        def _():
            at = pl.ds(r * owners, owners)
            pltpu.make_async_copy(qall.at[at], qall.at[at], q_recv_sem.at[r]).wait()

        @pl.when(i == requests)
        def _():
            at = pl.ds(r * owners, owners - 1)
            pltpu.make_async_copy(qall.at[at], qall.at[at], q_recv_sem.at[r]).wait()

        key_copy(r).wait()

    def score_tile(i, b, best, score):
        r = request_at(i)
        q = qall[pl.ds(r * owners, owners)].reshape(queries, HEAD_WIDTH)
        s = lax.dot_general(
            keys[r, b * KEY_TILE : (b + 1) * KEY_TILE, :],
            q,
            NT,
            preferred_element_type=F32,
        )
        for n in range(KEY_TILE // PAGE):
            p = b * (KEY_TILE // PAGE) + n
            left = lengths_ref[r] - slots_ref[r, p] * PAGE
            shown = jnp.where(
                row_in_page < left, s[n * PAGE : (n + 1) * PAGE], HIDDEN
            )
            score[p * PAGE : (p + 1) * PAGE, :] = shown
            high = jnp.max(shown.reshape(PAGE // 8, 8, queries), axis=0)
            best = high if best is None else jnp.maximum(best, high)
        return best

    def weigh_tile(i, b, state, score, top):
        r = request_at(i)
        acc, total = state
        w = jnp.exp2(score[b * KEY_TILE : (b + 1) * KEY_TILE, :] * scale2 - top)
        low = jnp.sum(w.reshape(KEY_TILE // 8, 8, queries), axis=0)
        added = lax.dot_general(
            values[r, b * KEY_TILE : (b + 1) * KEY_TILE, :],
            w.astype(BF16),
            TN,
            preferred_element_type=F32,
        )
        if acc is None:
            return added, low
        return acc + added, total + low

    def finish(i, state, top):
        acc, total = state
        total = jnp.maximum(jnp.sum(total, axis=0, keepdims=True), 1.0)
        out = (acc / total).T.astype(BF16)
        out_send[i - 1] = out.reshape(owners, block, HEAD_WIDTH)
        lse = top * (1.0 / math.log2(math.e)) + jnp.log(total)
        lse_send[i - 1] = jnp.concatenate(
            [lse[:, n * 128 : (n + 1) * 128] for n in range(queries // 128)], axis=0
        )

    def send_out(i):
        r = request_at(i)

        def send(peer_place):
            peer = r * owners + peer_place
            pltpu.make_async_remote_copy(
                src_ref=out_send.at[i - 1, peer_place],
                dst_ref=out_recv.at[me],
                send_sem=o_send_sem,
                recv_sem=o_recv_sem,
                device_id=(peer, head),
                device_id_type=pl.DeviceIdType.MESH,
            ).start()
            pltpu.make_async_remote_copy(
                src_ref=lse_send.at[i - 1],
                dst_ref=lse_recv.at[me],
                send_sem=l_send_sem,
                recv_sem=l_recv_sem,
                device_id=(peer, head),
                device_id_type=pl.DeviceIdType.MESH,
            ).start()

        for j in range(owners):
            place = (own_place + j) % owners
            if j == 0:

                @pl.when(i < requests)
                def _():
                    send(place)

            else:
                send(place)

    def half_step(i, now, after):
        score, top_ref = now
        wait_value = value_copy(request_at(i))
        wait_value.wait()
        top = jnp.max(top_ref[...], axis=0, keepdims=True) * scale2
        state = (None, None)
        best = None
        for b in range(tiles):
            if after is not None:
                best = score_tile(i + 1, b, best, after[0])
            state = weigh_tile(i, b, state, score, top)
        if after is not None:
            after[1][...] = best
        finish(i, state, top)
        send_out(i)

    a, b = (score_a, top_a), (score_b, top_b)
    wait_for(1)
    best = None
    for t in range(tiles):
        best = score_tile(1, t, best, score_a)
    top_a[...] = best

    def two_steps(n, _):
        i = 1 + 2 * n
        wait_for(i + 1)
        half_step(i, a, b)
        wait_for(i + 2)
        half_step(i + 1, b, a)
        return 0

    lax.fori_loop(0, requests // 2 - 1, two_steps, 0)
    wait_for(requests)
    half_step(requests - 1, a, b)
    half_step(requests, b, None)
    out_recv[me] = out_send[requests - 1, own_place]
    lse_recv[me] = lse_send[requests - 1]

    def arrived(ref, count, sem):
        at = pl.ds(0, count)
        pltpu.make_async_copy(ref.at[at], ref.at[at], sem).wait()

    arrived(lse_recv, n_seq - 1, l_recv_sem)
    per_line = 128 // block
    lse = lse_recv[:, pl.ds(own_place // per_line, 1), :].reshape(n_seq, 128)
    lse = pltpu.roll(lse, (128 - (own_place % per_line) * block) % 128, 1)
    best = jnp.maximum(jnp.max(lse, axis=0, keepdims=True), tree_lse)
    factor = jnp.exp(lse - best)
    tree_factor = jnp.exp(tree_lse - best)
    total = jnp.sum(factor, axis=0, keepdims=True) + tree_factor
    factor = jnp.concatenate(
        [factor / total, jnp.broadcast_to(tree_factor / total, (8, 128))], axis=0
    ).T[:block]
    for j in range(n_head):
        wo_copy(j).wait()
    arrived(out_recv, n_seq - 1, o_recv_sem)
    merged = tree_out * factor[:, n_seq : n_seq + 1]
    for n in range(n_seq):
        merged += out_recv[n].astype(F32) * factor[:, n : n + 1]
    merged = merged.astype(BF16)
    attended = jnp.concatenate(
        [merged[g * rows : (g + 1) * rows] for g in range(groups)], axis=1
    )

    def piece(j):
        return jnp.dot(attended, wo[j], preferred_element_type=F32)

    def part_copy(j):
        return pltpu.make_async_remote_copy(
            src_ref=part_send.at[j],
            dst_ref=part_recv.at[head],
            send_sem=p_send_sem,
            recv_sem=p_recv_sem,
            device_id=(me, j),
            device_id_type=pl.DeviceIdType.MESH,
        )

    order = sorted(range(1, n_head), key=lambda d: -min(d, n_head - d))
    for n, d in enumerate(order):
        j = (head + d) % n_head
        part_send[j] = piece(j).astype(BF16)
        if n > 0:
            part_copy((head + order[n - 1]) % n_head).start()
    mine = piece(head)
    part_copy((head + order[-1]) % n_head).start()
    at = pl.ds(pl.multiple_of(head * own_width, own_width), own_width)
    mine = mine + tokens_ref[:, at].astype(F32)
    part_recv[head] = jnp.zeros((rows, own_width), BF16)
    arrived(part_recv, n_head - 1, p_recv_sem)
    mixed_ref[...] = (mine + jnp.sum(part_recv[...].astype(F32), axis=0)).astype(BF16)

    arrived(part_send, n_head - 1, p_send_sem)
    arrived(qall, n_seq - 1, q_send_sem)
    arrived(kvtree, owners - 1, kv_send_sem)
    arrived(out_recv, n_seq - 1, o_send_sem)
    arrived(lse_recv, n_seq - 1, l_send_sem)


def per_device(
    tokens,
    norm_gain,
    w_query,
    key_projection,
    value_projection,
    w_out,
    cache_keys,
    paged_value_cache,
    lengths,
    parents,
    slot_block,
):
    n_seq = lax.axis_size("seq")
    n_head = lax.axis_size("head")
    rows, width = tokens.shape
    requests, context, _ = cache_keys.shape
    q_width = w_query.shape[1]
    groups = q_width // HEAD_WIDTH
    owners = TREE // rows
    block = groups * rows
    queries = owners * block
    own_width = width // n_head
    vmem = pl.BlockSpec(memory_space=pltpu.VMEM)
    smem = pl.BlockSpec(memory_space=pltpu.SMEM)
    hbm = pl.BlockSpec(memory_space=pl.ANY)
    dma = pltpu.SemaphoreType.DMA
    return pl.pallas_call(
        functools.partial(layer, n_seq, n_head),
        out_shape=jax.ShapeDtypeStruct((rows, own_width), BF16),
        in_specs=[smem, smem, vmem, vmem, vmem, hbm, hbm, hbm, hbm, hbm, hbm],
        out_specs=vmem,
        scratch_shapes=[
            pltpu.VMEM((width, q_width + 2 * HEAD_WIDTH), BF16),
            pltpu.VMEM((n_head, q_width, own_width), BF16),
            pltpu.VMEM((requests, context, HEAD_WIDTH), BF16),
            pltpu.VMEM((requests, context, HEAD_WIDTH), BF16),
            pltpu.VMEM((rows, width), BF16),
            pltpu.VMEM((n_seq, block, HEAD_WIDTH), BF16),
            pltpu.VMEM((owners, 2 * rows, HEAD_WIDTH), BF16),
            pltpu.VMEM((context, queries), F32),
            pltpu.VMEM((context, queries), F32),
            pltpu.VMEM((8, queries), F32),
            pltpu.VMEM((8, queries), F32),
            pltpu.VMEM((requests, owners, block, HEAD_WIDTH), BF16),
            pltpu.VMEM((requests, queries // 128, 128), F32),
            pltpu.VMEM((n_seq, block, HEAD_WIDTH), BF16),
            pltpu.VMEM((n_seq, queries // 128, 128), F32),
            pltpu.VMEM((n_head, rows, own_width), BF16),
            pltpu.VMEM((n_head, rows, own_width), BF16),
            dma((3, WEIGHT_PARTS)),
            dma((n_head,)),
            dma((requests,)),
            dma((requests,)),
            dma,
            dma((requests,)),
            dma,
            dma,
            dma,
            dma,
            dma,
            dma,
            dma,
            dma,
        ],
        compiler_params=pltpu.CompilerParams(
            collective_id=0,
            has_side_effects=True,
            vmem_limit_bytes=60 * 1024 * 1024,
        ),
        name="layer",
    )(
        lengths,
        slot_block,
        tokens,
        norm_gain.reshape(1, width),
        parents,
        w_query,
        key_projection,
        value_projection,
        w_out,
        cache_keys,
        paged_value_cache,
    )


def solution(mesh):
    in_specs = (
        P("seq", None),
        P(),
        P(None, "head"),
        P(None, "head"),
        P(None, "head"),
        P("head", None),
        P(None, "seq", "head"),
        P(None, "seq", "head"),
        P(),
        P(),
        P(None, "seq"),
    )
    return jax.shard_map(
        per_device,
        mesh=mesh,
        in_specs=in_specs,
        out_specs=P("seq", "head"),
        check_vma=False,
    )
```

```python
import functools
import math

import jax
import jax.numpy as jnp
from jax import lax
from jax.experimental import pallas as pl
from jax.experimental.pallas import tpu as pltpu
from jax.sharding import PartitionSpec as P

NORM_EPSILON = 1e-05
HIDDEN = -1e30
HEAD_WIDTH = 128
TREE = 64
PAGE = 128
KEY_TILE = 256
WEIGHT_PARTS = 4

NT = (((1,), (1,)), ((), ()))
TN = (((0,), (0,)), ((), ()))
F32 = jnp.float32
BF16 = jnp.bfloat16


def layer(
    n_seq,
    n_head,
    lengths_hbm,
    slots_hbm,
    tokens_hbm,
    gain_hbm,
    parents_hbm,
    wq_hbm,
    wk_hbm,
    wv_hbm,
    wo_hbm,
    keys_hbm,
    values_hbm,
    mixed_ref,
    lengths_ref,
    slots_ref,
    tokens_ref,
    gain_ref,
    parents_ref,
    small_sem,
    wqkv,
    wo,
    keys,
    values,
    normed,
    qall,
    kvtree,
    score_a,
    score_b,
    top_a,
    top_b,
    out_send,
    lse_send,
    out_recv,
    lse_recv,
    part_send,
    part_recv,
    w_sem,
    wo_sem,
    k_sem,
    v_sem,
    q_send_sem,
    q_recv_sem,
    kv_send_sem,
    kv_recv_sem,
    o_send_sem,
    o_recv_sem,
    l_send_sem,
    l_recv_sem,
    p_send_sem,
    p_recv_sem,
):
    me = lax.axis_index("seq")
    head = lax.axis_index("head")
    rows, width = tokens_ref.shape
    requests = keys.shape[0]
    context = keys.shape[1]
    owners = TREE // rows
    q_width = wq_hbm.shape[1]
    groups = q_width // HEAD_WIDTH
    block = groups * rows
    queries = owners * block
    tiles = context // KEY_TILE
    own_request = me // owners
    own_place = me % owners
    scale = HEAD_WIDTH**-0.5
    scale2 = scale * math.log2(math.e)

    barrier = pltpu.get_barrier_semaphore()

    def greet_seq(j, _):
        pl.semaphore_signal(
            barrier,
            inc=1,
            device_id=((me + j) % n_seq, head),
            device_id_type=pl.DeviceIdType.MESH,
        )
        return 0

    def greet_head(j, _):
        pl.semaphore_signal(
            barrier,
            inc=1,
            device_id=(me, (head + j) % n_head),
            device_id_type=pl.DeviceIdType.MESH,
        )
        return 0

    lax.fori_loop(1, n_seq, greet_seq, 0)
    lax.fori_loop(1, n_head, greet_head, 0)

    small = [
        pltpu.make_async_copy(source, target, small_sem.at[n])
        for n, (source, target) in enumerate(
            (
                (tokens_hbm, tokens_ref),
                (gain_hbm, gain_ref),
                (parents_hbm, parents_ref),
                (lengths_hbm, lengths_ref),
                (slots_hbm, slots_ref),
            )
        )
    ]
    for copy in small:
        copy.start()
    part = width // WEIGHT_PARTS

    def weight_copies(c):
        at = pl.ds(c * part, part)
        return (
            pltpu.make_async_copy(
                wq_hbm.at[at], wqkv.at[at, pl.ds(0, q_width)], w_sem.at[0, c]
            ),
            pltpu.make_async_copy(
                wk_hbm.at[at], wqkv.at[at, pl.ds(q_width, HEAD_WIDTH)], w_sem.at[1, c]
            ),
            pltpu.make_async_copy(
                wv_hbm.at[at],
                wqkv.at[at, pl.ds(q_width + HEAD_WIDTH, HEAD_WIDTH)],
                w_sem.at[2, c],
            ),
        )

    def key_copy(r):
        return pltpu.make_async_copy(keys_hbm.at[r], keys.at[r], k_sem.at[r])

    def value_copy(r):
        return pltpu.make_async_copy(values_hbm.at[r], values.at[r], v_sem.at[r])

    own_width = width // n_head

    def wo_copy(j):
        at = pl.ds(pl.multiple_of(j * own_width, own_width), own_width)
        return pltpu.make_async_copy(wo_hbm.at[:, at], wo.at[j], wo_sem.at[j])

    def request_at(i):
        return (own_request + i) % requests

    for c in range(WEIGHT_PARTS):
        for copy in weight_copies(c):
            copy.start()

    def start_cache(i, _):
        key_copy(request_at(i)).start()
        value_copy(request_at(i)).start()
        return 0

    def start_wo(j, _):
        wo_copy(j).start()
        return 0

    small[0].wait()
    small[1].wait()
    inputs = tokens_ref[...].astype(F32)
    mean = jnp.mean(inputs * inputs, axis=-1, keepdims=True)
    normed[...] = (
        inputs
        * lax.rsqrt(mean + NORM_EPSILON)
        * gain_ref[...].reshape(1, width).astype(F32)
    ).astype(BF16)

    for copy in small[2:]:
        copy.wait()
    parent = parents_ref[pl.ds(own_request, 1), :]
    node = lax.broadcasted_iota(jnp.int32, (TREE, TREE), 0)
    other = lax.broadcasted_iota(jnp.int32, (TREE, TREE), 1)
    reached = jnp.where((parent == node) | (node == other), 1.0, 0.0)
    for _ in range(max(1, (TREE - 1).bit_length())):
        half = reached.astype(BF16)
        reached = jnp.minimum(jnp.dot(half, half, preferred_element_type=F32), 1.0)

    projected = jnp.zeros((rows, wqkv.shape[1]), F32)
    for c in range(WEIGHT_PARTS):
        for copy in weight_copies(c):
            copy.wait()
        if c == WEIGHT_PARTS - 1:
            lax.fori_loop(1, requests + 1, start_cache, 0)
            lax.fori_loop(0, n_head, start_wo, 0)
        projected += jnp.dot(
            normed[:, c * part : (c + 1) * part],
            wqkv[c * part : (c + 1) * part, :],
            preferred_element_type=F32,
        )
    projected = projected.astype(BF16)
    for g in range(groups):
        qall[me, g * rows : (g + 1) * rows, :] = projected[
            :, g * HEAD_WIDTH : (g + 1) * HEAD_WIDTH
        ]
    for n in range(2):
        kvtree[own_place, n * rows : (n + 1) * rows, :] = projected[
            :, q_width + n * HEAD_WIDTH : q_width + (n + 1) * HEAD_WIDTH
        ]

    def q_copy(peer):
        return pltpu.make_async_remote_copy(
            src_ref=qall.at[me],
            dst_ref=qall.at[me],
            send_sem=q_send_sem,
            recv_sem=q_recv_sem.at[own_request],
            device_id=(peer, head),
            device_id_type=pl.DeviceIdType.MESH,
        )

    pl.semaphore_wait(barrier, n_seq - 1 + n_head - 1)

    def kv_send(j, _):
        peer = own_request * owners + (own_place + j) % owners
        pltpu.make_async_remote_copy(
            src_ref=kvtree.at[own_place],
            dst_ref=kvtree.at[own_place],
            send_sem=kv_send_sem,
            recv_sem=kv_recv_sem,
            device_id=(peer, head),
            device_id_type=pl.DeviceIdType.MESH,
        ).start()
        return 0

    def q_send(n, _):
        to = (own_request + requests - 1 - n // owners) % requests
        q_copy(to * owners + (own_place + n) % owners).start()
        return 0

    def q_send_own(j, _):
        q_copy(own_request * owners + (own_place + j) % owners).start()
        return 0

    lax.fori_loop(0, owners, q_send, 0)
    lax.fori_loop(1, owners, kv_send, 0)
    lax.fori_loop(owners, (requests - 1) * owners, q_send, 0)
    lax.fori_loop(1, owners, q_send_own, 0)

    pltpu.make_async_copy(
        kvtree.at[pl.ds(0, owners - 1)], kvtree.at[pl.ds(0, owners - 1)], kv_recv_sem
    ).wait()
    lanes = 128
    own_queries = qall[me]
    own_queries = jnp.concatenate([own_queries] * (lanes // block), axis=0)
    tree_keys = kvtree[:, :rows, :].reshape(TREE, HEAD_WIDTH)
    tree_values = kvtree[:, rows:, :].reshape(TREE, HEAD_WIDTH)
    token = lax.broadcasted_iota(jnp.int32, (TREE, lanes), 0)
    lane = lax.broadcasted_iota(jnp.int32, (TREE, lanes), 1)
    pick = jnp.where(token == own_place * rows + lane % rows, 1.0, 0.0).astype(BF16)
    seen = jnp.dot(reached.astype(BF16), pick, preferred_element_type=F32) > 0.5
    tree_scores = lax.dot_general(
        tree_keys, own_queries, NT, preferred_element_type=F32
    )
    tree_scores = jnp.where(seen, tree_scores, HIDDEN)
    tree_top = jnp.max(tree_scores, axis=0, keepdims=True)
    tree_weights = jnp.where(
        seen, jnp.exp2(tree_scores * scale2 - tree_top * scale2), 0.0
    )
    tree_total = jnp.maximum(jnp.sum(tree_weights, axis=0, keepdims=True), 1.0)
    tree_sum = lax.dot_general(
        tree_values, tree_weights.astype(BF16), TN, preferred_element_type=F32
    )
    tree_out = (tree_sum / tree_total).astype(BF16).astype(F32).T[:block]
    tree_lse = tree_top * scale + jnp.log(tree_total)

    row_in_page = lax.broadcasted_iota(jnp.int32, (PAGE, queries), 0)

    def wait_for(i):
        r = request_at(i)

        @pl.when(i < requests)
        def _():
            at = pl.ds(r * owners, owners)
            pltpu.make_async_copy(qall.at[at], qall.at[at], q_recv_sem.at[r]).wait()

        @pl.when(i == requests)
        def _():
            at = pl.ds(r * owners, owners - 1)
            pltpu.make_async_copy(qall.at[at], qall.at[at], q_recv_sem.at[r]).wait()

        key_copy(r).wait()

    def score_tile(i, b, best, score):
        r = request_at(i)
        q = qall[pl.ds(r * owners, owners)].reshape(queries, HEAD_WIDTH)
        s = lax.dot_general(
            keys[r, b * KEY_TILE : (b + 1) * KEY_TILE, :],
            q,
            NT,
            preferred_element_type=F32,
        )
        for n in range(KEY_TILE // PAGE):
            p = b * (KEY_TILE // PAGE) + n
            left = lengths_ref[r] - slots_ref[r, p] * PAGE
            shown = jnp.where(
                row_in_page < left, s[n * PAGE : (n + 1) * PAGE], HIDDEN
            )
            score[p * PAGE : (p + 1) * PAGE, :] = shown
            high = jnp.max(shown.reshape(PAGE // 8, 8, queries), axis=0)
            best = high if best is None else jnp.maximum(best, high)
        return best

    def weigh_tile(i, b, state, score, top):
        r = request_at(i)
        acc, total = state
        w = jnp.exp2(score[b * KEY_TILE : (b + 1) * KEY_TILE, :] * scale2 - top)
        low = jnp.sum(w.reshape(KEY_TILE // 8, 8, queries), axis=0)
        added = lax.dot_general(
            values[r, b * KEY_TILE : (b + 1) * KEY_TILE, :],
            w.astype(BF16),
            TN,
            preferred_element_type=F32,
        )
        if acc is None:
            return added, low
        return acc + added, total + low

    def finish(i, state, top):
        acc, total = state
        total = jnp.maximum(jnp.sum(total, axis=0, keepdims=True), 1.0)
        out = (acc / total).T.astype(BF16)
        out_send[i - 1] = out.reshape(owners, block, HEAD_WIDTH)
        lse = top * (1.0 / math.log2(math.e)) + jnp.log(total)
        lse_send[i - 1] = jnp.concatenate(
            [lse[:, n * 128 : (n + 1) * 128] for n in range(queries // 128)], axis=0
        )

    def send_out(i):
        r = request_at(i)

        def send(peer_place):
            peer = r * owners + peer_place
            pltpu.make_async_remote_copy(
                src_ref=out_send.at[i - 1, peer_place],
                dst_ref=out_recv.at[me],
                send_sem=o_send_sem,
                recv_sem=o_recv_sem,
                device_id=(peer, head),
                device_id_type=pl.DeviceIdType.MESH,
            ).start()
            pltpu.make_async_remote_copy(
                src_ref=lse_send.at[i - 1],
                dst_ref=lse_recv.at[me],
                send_sem=l_send_sem,
                recv_sem=l_recv_sem,
                device_id=(peer, head),
                device_id_type=pl.DeviceIdType.MESH,
            ).start()

        for j in range(owners):
            place = (own_place + j) % owners
            if j == 0:

                @pl.when(i < requests)
                def _():
                    send(place)

            else:
                send(place)

    def half_step(i, now, after):
        score, top_ref = now
        wait_value = value_copy(request_at(i))
        wait_value.wait()
        top = jnp.max(top_ref[...], axis=0, keepdims=True) * scale2
        state = (None, None)
        best = None
        for b in range(tiles):
            if after is not None:
                best = score_tile(i + 1, b, best, after[0])
            state = weigh_tile(i, b, state, score, top)
        if after is not None:
            after[1][...] = best
        finish(i, state, top)
        send_out(i)

    a, b = (score_a, top_a), (score_b, top_b)
    wait_for(1)
    best = None
    for t in range(tiles):
        best = score_tile(1, t, best, score_a)
    top_a[...] = best

    def two_steps(n, _):
        i = 1 + 2 * n
        wait_for(i + 1)
        half_step(i, a, b)
        wait_for(i + 2)
        half_step(i + 1, b, a)
        return 0

    lax.fori_loop(0, requests // 2 - 1, two_steps, 0)
    wait_for(requests)
    half_step(requests - 1, a, b)
    half_step(requests, b, None)
    out_recv[me] = out_send[requests - 1, own_place]
    lse_recv[me] = lse_send[requests - 1]

    def arrived(ref, count, sem):
        at = pl.ds(0, count)
        pltpu.make_async_copy(ref.at[at], ref.at[at], sem).wait()

    arrived(lse_recv, n_seq - 1, l_recv_sem)
    per_line = 128 // block
    lse = lse_recv[:, pl.ds(own_place // per_line, 1), :].reshape(n_seq, 128)
    lse = pltpu.roll(lse, (128 - (own_place % per_line) * block) % 128, 1)
    best = jnp.maximum(jnp.max(lse, axis=0, keepdims=True), tree_lse)
    factor = jnp.exp(lse - best)
    tree_factor = jnp.exp(tree_lse - best)
    total = jnp.sum(factor, axis=0, keepdims=True) + tree_factor
    factor = jnp.concatenate(
        [factor / total, jnp.broadcast_to(tree_factor / total, (8, 128))], axis=0
    ).T[:block]
    for j in range(n_head):
        wo_copy(j).wait()
    arrived(out_recv, n_seq - 1, o_recv_sem)
    merged = tree_out * factor[:, n_seq : n_seq + 1]
    for n in range(n_seq):
        merged += out_recv[n].astype(F32) * factor[:, n : n + 1]
    merged = merged.astype(BF16)
    attended = jnp.concatenate(
        [merged[g * rows : (g + 1) * rows] for g in range(groups)], axis=1
    )

    def piece(j):
        return jnp.dot(attended, wo[j], preferred_element_type=F32)

    def part_copy(j):
        return pltpu.make_async_remote_copy(
            src_ref=part_send.at[j],
            dst_ref=part_recv.at[head],
            send_sem=p_send_sem,
            recv_sem=p_recv_sem,
            device_id=(me, j),
            device_id_type=pl.DeviceIdType.MESH,
        )

    order = sorted(range(1, n_head), key=lambda d: -min(d, n_head - d))
    for n, d in enumerate(order):
        j = (head + d) % n_head
        part_send[j] = piece(j).astype(BF16)
        if n > 0:
            part_copy((head + order[n - 1]) % n_head).start()
    mine = piece(head)
    part_copy((head + order[-1]) % n_head).start()
    at = pl.ds(pl.multiple_of(head * own_width, own_width), own_width)
    mine = mine + tokens_ref[:, at].astype(F32)
    part_recv[head] = jnp.zeros((rows, own_width), BF16)
    arrived(part_recv, n_head - 1, p_recv_sem)
    mixed_ref[...] = (mine + jnp.sum(part_recv[...].astype(F32), axis=0)).astype(BF16)

    arrived(part_send, n_head - 1, p_send_sem)
    arrived(qall, n_seq - 1, q_send_sem)
    arrived(kvtree, owners - 1, kv_send_sem)
    arrived(out_recv, n_seq - 1, o_send_sem)
    arrived(lse_recv, n_seq - 1, l_send_sem)


def per_device(
    tokens,
    norm_gain,
    w_query,
    key_projection,
    value_projection,
    w_out,
    cache_keys,
    paged_value_cache,
    lengths,
    parents,
    slot_block,
):
    n_seq = lax.axis_size("seq")
    n_head = lax.axis_size("head")
    rows, width = tokens.shape
    requests, context, _ = cache_keys.shape
    q_width = w_query.shape[1]
    groups = q_width // HEAD_WIDTH
    owners = TREE // rows
    block = groups * rows
    queries = owners * block
    own_width = width // n_head
    vmem = pl.BlockSpec(memory_space=pltpu.VMEM)
    hbm = pl.BlockSpec(memory_space=pltpu.HBM)
    dma = pltpu.SemaphoreType.DMA
    return pl.pallas_call(
        functools.partial(layer, n_seq, n_head),
        out_shape=pltpu.VMEM((rows, own_width), BF16),
        in_specs=[hbm] * 11,
        out_specs=vmem,
        scratch_shapes=[
            pltpu.SMEM(lengths.shape, jnp.int32),
            pltpu.SMEM(slot_block.shape, jnp.int32),
            pltpu.VMEM(tokens.shape, BF16),
            pltpu.VMEM(norm_gain.shape, BF16),
            pltpu.VMEM(parents.shape, jnp.int32),
            dma((5,)),
            pltpu.VMEM((width, q_width + 2 * HEAD_WIDTH), BF16),
            pltpu.VMEM((n_head, q_width, own_width), BF16),
            pltpu.VMEM((requests, context, HEAD_WIDTH), BF16),
            pltpu.VMEM((requests, context, HEAD_WIDTH), BF16),
            pltpu.VMEM((rows, width), BF16),
            pltpu.VMEM((n_seq, block, HEAD_WIDTH), BF16),
            pltpu.VMEM((owners, 2 * rows, HEAD_WIDTH), BF16),
            pltpu.VMEM((context, queries), F32),
            pltpu.VMEM((context, queries), F32),
            pltpu.VMEM((8, queries), F32),
            pltpu.VMEM((8, queries), F32),
            pltpu.VMEM((requests, owners, block, HEAD_WIDTH), BF16),
            pltpu.VMEM((requests, queries // 128, 128), F32),
            pltpu.VMEM((n_seq, block, HEAD_WIDTH), BF16),
            pltpu.VMEM((n_seq, queries // 128, 128), F32),
            pltpu.VMEM((n_head, rows, own_width), BF16),
            pltpu.VMEM((n_head, rows, own_width), BF16),
            dma((3, WEIGHT_PARTS)),
            dma((n_head,)),
            dma((requests,)),
            dma((requests,)),
            dma,
            dma((requests,)),
            dma,
            dma,
            dma,
            dma,
            dma,
            dma,
            dma,
            dma,
        ],
        compiler_params=pltpu.CompilerParams(
            collective_id=0,
            has_side_effects=True,
            vmem_limit_bytes=60 * 1024 * 1024,
        ),
        name="layer",
    )(
        lengths,
        slot_block,
        tokens,
        norm_gain,
        parents,
        w_query,
        key_projection,
        value_projection,
        w_out,
        cache_keys,
        paged_value_cache,
    )


def solution(mesh):
    in_specs = (
        P("seq", None),
        P(),
        P(None, "head"),
        P(None, "head"),
        P(None, "head"),
        P("head", None),
        P(None, "seq", "head"),
        P(None, "seq", "head"),
        P(),
        P(),
        P(None, "seq"),
    )
    return jax.shard_map(
        per_device,
        mesh=mesh,
        in_specs=in_specs,
        out_specs=P("seq", "head"),
        check_vma=False,
    )
```

```python
import functools
import math

import jax
import jax.numpy as jnp
from jax import lax
from jax.experimental import pallas as pl
from jax.experimental.pallas import tpu as pltpu
from jax.sharding import PartitionSpec as P

NORM_EPSILON = 1e-05
HIDDEN = -1e30
HEAD_WIDTH = 128
TREE = 64
PAGE = 128
KEY_TILE = 256
WEIGHT_PARTS = 4
ORDER = ((0, 1), (1, 0), (2, 0), (2, 1), (3, 1), (1, 1), (3, 0), (0, 0))

NT = (((1,), (1,)), ((), ()))
TN = (((0,), (0,)), ((), ()))
F32 = jnp.float32
BF16 = jnp.bfloat16


def layer(
    n_seq,
    n_head,
    lengths_hbm,
    slots_hbm,
    tokens_hbm,
    gain_hbm,
    parents_hbm,
    wq_hbm,
    wk_hbm,
    wv_hbm,
    wo_hbm,
    keys_hbm,
    values_hbm,
    mixed_ref,
    lengths_ref,
    slots_ref,
    tokens_ref,
    gain_ref,
    parents_ref,
    small_sem,
    wqkv,
    wo,
    keys,
    values,
    normed,
    qall,
    kvtree,
    score_a,
    score_b,
    top_a,
    top_b,
    out_own,
    lse_own,
    out_swap,
    lse_swap,
    out_pair,
    lse_pair,
    out_last,
    out_recv,
    lse_recv,
    part_send,
    part_recv,
    w_sem,
    wo_sem,
    cache_sem,
    q_send_sem,
    q_far_sem,
    q_near_sem,
    kv_send_sem,
    kv_recv_sem,
    x_send_sem,
    x_recv_sem,
    xl_send_sem,
    xl_recv_sem,
    o_send_sem,
    o_recv_sem,
    l_send_sem,
    l_recv_sem,
    p_send_sem,
    p_recv_sem,
):
    me = lax.axis_index("seq")
    head = lax.axis_index("head")
    rows, width = tokens_ref.shape
    requests = keys.shape[0]
    context = keys.shape[1]
    owners = TREE // rows
    q_width = wq_hbm.shape[1]
    groups = q_width // HEAD_WIDTH
    block = groups * rows
    queries = owners * block
    tiles = context // KEY_TILE
    own_request = me // owners
    own_place = me % owners
    scale = HEAD_WIDTH**-0.5
    scale2 = scale * math.log2(math.e)

    small = [
        pltpu.make_async_copy(source, target, small_sem.at[n])
        for n, (source, target) in enumerate(
            (
                (tokens_hbm, tokens_ref),
                (gain_hbm, gain_ref),
                (parents_hbm, parents_ref),
                (lengths_hbm, lengths_ref),
                (slots_hbm, slots_ref),
            )
        )
    ]
    for copy in small[:2]:
        copy.start()
    part = width // WEIGHT_PARTS

    wide = 2 * HEAD_WIDTH
    pieces = q_width // wide

    def start_weights(source, first, column, sem):
        for c in range(WEIGHT_PARTS):
            at = pl.ds(c * part, part)
            count = min(wide, source.shape[1])
            pltpu.make_async_copy(
                source.at[at, pl.ds(first, count)],
                wqkv.at[at, pl.ds(column, count)],
                w_sem.at[sem],
            ).start()

    def project(n):
        at = wqkv.at[:, pl.ds(n * wide, wide)]
        pltpu.make_async_copy(at, at, w_sem.at[n]).wait()
        return jnp.dot(
            normed[...],
            wqkv[:, n * wide : (n + 1) * wide],
            preferred_element_type=F32,
        ).astype(BF16)

    own_width = width // n_head

    def wo_copy(j):
        at = pl.ds(pl.multiple_of(j * own_width, own_width), own_width)
        return pltpu.make_async_copy(wo_hbm.at[:, at], wo.at[j], wo_sem)

    core = own_place % 2
    spot = own_place // 2
    chip = me // 2
    partner = me + 1 - 2 * core
    lanes = 128
    chips = n_seq // 2
    chips_x = 2
    joined = requests - 2
    unforwarded = 1

    rows_y = requests // chips_x

    def request_at(i):
        y = (own_request // chips_x + ORDER[i][0]) % rows_y
        return y * chips_x + (own_request + ORDER[i][1]) % chips_x

    def user_at(i):
        y = (own_request // chips_x + rows_y - ORDER[i][0]) % rows_y
        return y * chips_x + (own_request + ORDER[i][1]) % chips_x

    start_weights(wq_hbm, 0, 0, 0)

    barrier = pltpu.get_barrier_semaphore()

    def greet_seq(j, _):
        pl.semaphore_signal(
            barrier,
            inc=1,
            device_id=((me + j) % n_seq, head),
            device_id_type=pl.DeviceIdType.MESH,
        )
        return 0

    def greet_head(j, _):
        pl.semaphore_signal(
            barrier,
            inc=1,
            device_id=(me, (head + j) % n_head),
            device_id_type=pl.DeviceIdType.MESH,
        )
        return 0

    for n in sorted(range(1, n_head), key=lambda d: -min(d, n_head - d)):
        greet_head(n, 0)
    lax.fori_loop(1, n_seq, greet_seq, 0)

    for n in range(1, pieces):
        start_weights(wq_hbm, n * wide, n * wide, n)
    for copy in small[2:]:
        copy.start()

    def start_wo(j, _):
        wo_copy(j).start()
        return 0

    small[0].wait()
    small[1].wait()
    inputs = tokens_ref[...].astype(F32)
    mean = jnp.mean(inputs * inputs, axis=-1, keepdims=True)
    normed[...] = (
        inputs
        * lax.rsqrt(mean + NORM_EPSILON)
        * gain_ref[...].reshape(1, width).astype(F32)
    ).astype(BF16)

    for n in range(pieces):
        projected = project(n)
        if n == 0:
            start_weights(wk_hbm, 0, q_width, pieces)
            start_weights(wv_hbm, 0, q_width + HEAD_WIDTH, pieces)
        for g in range(2):
            line = (n * 2 + g) * rows
            qall[me, line : line + rows, :] = projected[
                :, g * HEAD_WIDTH : (g + 1) * HEAD_WIDTH
            ]

    def remote(source, target, send_sem, recv_sem, peer):
        return pltpu.make_async_remote_copy(
            src_ref=source,
            dst_ref=target,
            send_sem=send_sem,
            recv_sem=recv_sem,
            device_id=(peer, head),
            device_id_type=pl.DeviceIdType.MESH,
        )

    def arrived(ref, count, sem):
        at = pl.ds(0, count)
        pltpu.make_async_copy(ref.at[at], ref.at[at], sem).wait()

    def q_copy(which, recv_sem, peer):
        return remote(qall.at[which], qall.at[which], q_send_sem, recv_sem, peer)

    pl.semaphore_wait(barrier, n_seq - 1 + n_head - 1)

    def q_send(i):
        for n in range(2):
            to = user_at(i) * owners + (spot + n) % 2 * 2
            q_copy(me, q_far_sem.at[own_request], to + core).start()
            if i < unforwarded:
                q_copy(me, q_near_sem.at[own_request], to + 1 - core).start()

    q_send(0)
    q_send(1)
    for i in range(requests):
        r = request_at(i)
        for source, target in ((keys_hbm, keys), (values_hbm, values)):
            pltpu.make_async_copy(source.at[r], target.at[r], cache_sem.at[r]).start()
    lax.fori_loop(0, n_head, start_wo, 0)

    projected = project(pieces)
    for n in range(2):
        kvtree[own_place, n * rows : (n + 1) * rows, :] = projected[
            :, n * HEAD_WIDTH : (n + 1) * HEAD_WIDTH
        ]

    q_send(2)
    q_send(3)

    for copy in small[2:]:
        copy.wait()
    parent = parents_ref[pl.ds(own_request, 1), :]
    node = lax.broadcasted_iota(jnp.int32, (TREE, TREE), 0)
    other = lax.broadcasted_iota(jnp.int32, (TREE, TREE), 1)
    reached = jnp.where((parent == node) | (node == other), 1.0, 0.0)
    for _ in range(max(1, (TREE - 1).bit_length())):
        half = reached.astype(BF16)
        reached = jnp.minimum(jnp.dot(half, half, preferred_element_type=F32), 1.0)

    for n in range(1, owners):
        peer = own_request * owners + (own_place + n) % owners
        mine = kvtree.at[own_place]
        remote(mine, mine, kv_send_sem, kv_recv_sem, peer).start()
    q_send(4)
    q_send(5)

    row_in_page = lax.broadcasted_iota(jnp.int32, (PAGE, queries), 0)

    def forward(i):
        r = request_at(i)
        base = r * owners + core
        if i == requests - 1:
            arrived(qall, 1, q_far_sem.at[r])
            q_copy(beside, q_near_sem.at[r], partner).start()
        else:
            arrived(qall, 2, q_far_sem.at[r])
            q_copy(base, q_near_sem.at[r], partner).start()
            q_copy(base + 2, q_near_sem.at[r], partner).start()

    def wait_for(i):
        r = request_at(i)
        if i < unforwarded:
            arrived(qall, 2, q_far_sem.at[r])
        arrived(qall, 2, q_near_sem.at[r])
        arrived(keys, 2, cache_sem.at[r])

    def score_tile(i, b, best, score):
        r = request_at(i)
        q = qall[pl.ds(r * owners, owners)].reshape(queries, HEAD_WIDTH)
        s = lax.dot_general(
            keys[r, b * KEY_TILE : (b + 1) * KEY_TILE, :],
            q,
            NT,
            preferred_element_type=F32,
        )
        for n in range(KEY_TILE // PAGE):
            p = b * (KEY_TILE // PAGE) + n
            left = lengths_ref[r] - slots_ref[r, p] * PAGE
            shown = jnp.where(
                row_in_page < left, s[n * PAGE : (n + 1) * PAGE], HIDDEN
            )
            score[p * PAGE : (p + 1) * PAGE, :] = shown
            high = jnp.max(shown.reshape(PAGE // 8, 8, queries), axis=0)
            best = high if best is None else jnp.maximum(best, high)
        return best

    def weigh_tile(i, b, state, score, top):
        r = request_at(i)
        acc, total = state
        w = jnp.exp2(score[b * KEY_TILE : (b + 1) * KEY_TILE, :] * scale2 - top)
        low = jnp.sum(w.reshape(KEY_TILE // 8, 8, queries), axis=0)
        added = lax.dot_general(
            values[r, b * KEY_TILE : (b + 1) * KEY_TILE, :],
            w.astype(BF16),
            TN,
            preferred_element_type=F32,
        )
        if acc is None:
            return added, low
        return acc + added, total + low

    def finish(i, state, top, last):
        acc, total = state
        total = jnp.maximum(jnp.sum(total, axis=0, keepdims=True), 1.0)
        out = acc / total
        lse = top * (1.0 / math.log2(math.e)) + jnp.log(total)
        for n in range(2):
            half = slice(n * lanes, (n + 1) * lanes)
            lse_own[i, n] = lse[:, half]
            if not last:
                out_own[i, n] = out[:, half].astype(BF16)
        if last:
            out = out.T.astype(BF16).reshape(owners, block, HEAD_WIDTH)
            out_last[i - joined] = out

    def swap(i):
        other = 1 - core
        remote(
            out_own.at[i, other], out_swap.at[i], x_send_sem, x_recv_sem.at[i], partner
        ).start()
        remote(
            lse_own.at[i, other],
            lse_swap.at[i],
            xl_send_sem,
            xl_recv_sem.at[i],
            partner,
        ).start()

    def wait_swap(i):
        arrived(out_swap, 1, x_recv_sem.at[i])
        arrived(lse_swap, 1, xl_recv_sem.at[i])

    def join(i):
        mine, theirs = lse_own[i, core], lse_swap[i]
        high = jnp.maximum(mine, theirs)
        mine = jnp.exp(mine - high)
        theirs = jnp.exp(theirs - high)
        total = mine + theirs
        out = out_own[i, core].astype(F32) * (mine / total)
        out += out_swap[i].astype(F32) * (theirs / total)
        out_pair[i] = out.T.astype(BF16).reshape(2, block, HEAD_WIDTH)
        lse_pair[i] = high + jnp.log(total)

    def send_pair(i):
        first = request_at(i) * owners + core * 2

        for n in range(2):
            place = (core + n) % 2
            peer = first + place
            remote(
                out_pair.at[i, place], out_recv.at[chip], o_send_sem, o_recv_sem, peer
            ).start()
            remote(
                lse_pair.at[i], lse_recv.at[chip], l_send_sem, l_recv_sem, peer
            ).start()

    def send_direct(i):
        r = request_at(i)
        own = i == requests - 1
        spare = chips + (i - joined) * 2 + chip % 2
        slot = chip * (1 - core) + spare * core

        def send(n, _):
            place = (own_place + n) % owners
            peer = r * owners + place
            remote(
                out_last.at[i - joined, place],
                out_recv.at[slot],
                o_send_sem,
                o_recv_sem,
                peer,
            ).start()
            remote(
                lse_own.at[i, place // 2],
                lse_recv.at[slot],
                l_send_sem,
                l_recv_sem,
                peer,
            ).start()
            return 0

        lax.fori_loop(1 if own else 0, owners, send, 0)
        if own:
            out_recv[slot] = out_last[i - joined, own_place]
            lse_recv[slot] = lse_own[i, spot]

    def half_step(i, now, after):
        joins = i >= 2
        direct = i >= joined
        if i == 0:
            forward(1)
        if i + 2 < requests:
            forward(i + 2)
        if after is not None:
            wait_for(i + 1)
        if joins:
            wait_swap(i - 2)
        score, top_ref = now
        top = jnp.max(top_ref[...], axis=0, keepdims=True) * scale2
        state = (None, None)
        best = None
        for b in range(tiles):
            if after is not None:
                best = score_tile(i + 1, b, best, after[0])
            state = weigh_tile(i, b, state, score, top)
        if after is not None:
            after[1][...] = best
        finish(i, state, top, direct)
        if joins:
            join(i - 2)
        if direct:
            send_direct(i)
        else:
            swap(i)
        if joins:
            send_pair(i - 2)

    a, b = (score_a, top_a), (score_b, top_b)
    wait_for(0)
    best = None
    for t in range(tiles):
        best = score_tile(0, t, best, score_a)
    top_a[...] = best
    q_send(6)
    q_copy(me, q_near_sem.at[own_request], partner).start()
    beside = own_request * owners + (1 - spot) * 2 + core
    q_copy(me, q_far_sem.at[own_request], beside).start()
    for n in range(requests // 2):
        for i, now, after in ((2 * n, a, b), (2 * n + 1, b, a)):
            half_step(i, now, after if i < requests - 1 else None)

    arrived(kvtree, owners - 1, kv_recv_sem)
    own_queries = qall[me]
    own_queries = jnp.concatenate([own_queries] * (lanes // block), axis=0)
    tree_keys = kvtree[:, :rows, :].reshape(TREE, HEAD_WIDTH)
    tree_values = kvtree[:, rows:, :].reshape(TREE, HEAD_WIDTH)
    token = lax.broadcasted_iota(jnp.int32, (TREE, lanes), 0)
    lane = lax.broadcasted_iota(jnp.int32, (TREE, lanes), 1)
    pick = jnp.where(token == own_place * rows + lane % rows, 1.0, 0.0).astype(BF16)
    seen = jnp.dot(reached.astype(BF16), pick, preferred_element_type=F32) > 0.5
    tree_scores = lax.dot_general(
        tree_keys, own_queries, NT, preferred_element_type=F32
    )
    tree_scores = jnp.where(seen, tree_scores, HIDDEN)
    tree_top = jnp.max(tree_scores, axis=0, keepdims=True)
    tree_weights = jnp.where(
        seen, jnp.exp2(tree_scores * scale2 - tree_top * scale2), 0.0
    )
    tree_total = jnp.maximum(jnp.sum(tree_weights, axis=0, keepdims=True), 1.0)
    tree_sum = lax.dot_general(
        tree_values, tree_weights.astype(BF16), TN, preferred_element_type=F32
    )
    blocks = chips + 2 * (requests - joined)
    out_recv[blocks] = (tree_sum / tree_total).T[:block].astype(BF16)
    lse_recv[blocks] = tree_top * scale + jnp.log(tree_total)
    for n in range(blocks + 1, lse_recv.shape[0]):
        lse_recv[n] = jnp.full((1, lanes), HIDDEN, F32)
    arrived(wo, n_head, wo_sem)

    arrived(lse_recv, blocks - 1, l_recv_sem)
    lse = lse_recv[...].reshape(lse_recv.shape[0], lanes)
    lse = pltpu.roll(lse, (lanes - core * block) % lanes, 1)
    factor = jnp.exp(lse - jnp.max(lse, axis=0, keepdims=True))
    factor = (factor / jnp.sum(factor, axis=0, keepdims=True)).T[:block]
    arrived(out_recv, blocks - 1, o_recv_sem)
    merged = jnp.zeros((block, HEAD_WIDTH), F32)
    for n in range(blocks + 1):
        merged += out_recv[n].astype(F32) * factor[:, n : n + 1]
    merged = merged.astype(BF16)
    attended = jnp.concatenate(
        [merged[g * rows : (g + 1) * rows] for g in range(groups)], axis=1
    )

    def piece(j):
        return jnp.dot(attended, wo[j], preferred_element_type=F32)

    def part_copy(j):
        return pltpu.make_async_remote_copy(
            src_ref=part_send.at[j],
            dst_ref=part_recv.at[head],
            send_sem=p_send_sem,
            recv_sem=p_recv_sem,
            device_id=(me, j),
            device_id_type=pl.DeviceIdType.MESH,
        )

    order = sorted(range(1, n_head), key=lambda d: -min(d, n_head - d))
    for n, d in enumerate(order):
        j = (head + d) % n_head
        part_send[j] = piece(j).astype(BF16)
        if n > 0:
            part_copy((head + order[n - 1]) % n_head).start()
    mine = piece(head)
    part_copy((head + order[-1]) % n_head).start()
    at = pl.ds(pl.multiple_of(head * own_width, own_width), own_width)
    mine = mine + tokens_ref[:, at].astype(F32)
    part_recv[head] = jnp.zeros((rows, own_width), BF16)
    arrived(part_recv, n_head - 1, p_recv_sem)
    mixed_ref[...] = (mine + jnp.sum(part_recv[...].astype(F32), axis=0)).astype(BF16)

    arrived(part_send, n_head - 1, p_send_sem)
    arrived(qall, n_seq - 1, q_send_sem)
    arrived(kvtree, owners - 1, kv_send_sem)
    arrived(out_swap, joined, x_send_sem)
    arrived(lse_swap, joined, xl_send_sem)
    arrived(out_recv, blocks - 1, o_send_sem)
    arrived(lse_recv, blocks - 1, l_send_sem)


def per_device(
    tokens,
    norm_gain,
    w_query,
    key_projection,
    value_projection,
    w_out,
    cache_keys,
    paged_value_cache,
    lengths,
    parents,
    slot_block,
):
    n_seq = lax.axis_size("seq")
    n_head = lax.axis_size("head")
    rows, width = tokens.shape
    requests, context, _ = cache_keys.shape
    q_width = w_query.shape[1]
    groups = q_width // HEAD_WIDTH
    owners = TREE // rows
    block = groups * rows
    queries = owners * block
    own_width = width // n_head
    vmem = pl.BlockSpec(memory_space=pltpu.VMEM)
    hbm = pl.BlockSpec(memory_space=pltpu.HBM)
    dma = pltpu.SemaphoreType.DMA
    return pl.pallas_call(
        functools.partial(layer, n_seq, n_head),
        out_shape=pltpu.VMEM((rows, own_width), BF16),
        in_specs=[hbm] * 11,
        out_specs=vmem,
        scratch_shapes=[
            pltpu.SMEM(lengths.shape, jnp.int32),
            pltpu.SMEM(slot_block.shape, jnp.int32),
            pltpu.VMEM(tokens.shape, BF16),
            pltpu.VMEM(norm_gain.shape, BF16),
            pltpu.VMEM(parents.shape, jnp.int32),
            dma((5,)),
            pltpu.VMEM((width, q_width + 2 * HEAD_WIDTH), BF16),
            pltpu.VMEM((n_head, q_width, own_width), BF16),
            pltpu.VMEM((requests, context, HEAD_WIDTH), BF16),
            pltpu.VMEM((requests, context, HEAD_WIDTH), BF16),
            pltpu.VMEM((rows, width), BF16),
            pltpu.VMEM((n_seq, block, HEAD_WIDTH), BF16),
            pltpu.VMEM((owners, 2 * rows, HEAD_WIDTH), BF16),
            pltpu.VMEM((context, queries), F32),
            pltpu.VMEM((context, queries), F32),
            pltpu.VMEM((8, queries), F32),
            pltpu.VMEM((8, queries), F32),
            pltpu.VMEM((requests, 2, HEAD_WIDTH, 2 * block), BF16),
            pltpu.VMEM((requests, 2, 1, 2 * block), F32),
            pltpu.VMEM((requests, HEAD_WIDTH, 2 * block), BF16),
            pltpu.VMEM((requests, 1, 2 * block), F32),
            pltpu.VMEM((requests, 2, block, HEAD_WIDTH), BF16),
            pltpu.VMEM((requests, 1, 2 * block), F32),
            pltpu.VMEM((2, owners, block, HEAD_WIDTH), BF16),
            pltpu.VMEM((24, block, HEAD_WIDTH), BF16),
            pltpu.VMEM((24, 1, 2 * block), F32),
            pltpu.VMEM((n_head, rows, own_width), BF16),
            pltpu.VMEM((n_head, rows, own_width), BF16),
            dma((q_width // (2 * HEAD_WIDTH) + 1,)),
            dma,
            dma((requests,)),
            dma,
            dma((requests,)),
            dma((requests,)),
            dma,
            dma,
            dma,
            dma((requests - 2,)),
            dma,
            dma((requests - 2,)),
            dma,
            dma,
            dma,
            dma,
            dma,
            dma,
        ],
        compiler_params=pltpu.CompilerParams(
            collective_id=0,
            has_side_effects=True,
            vmem_limit_bytes=60 * 1024 * 1024,
        ),
        name="layer",
    )(
        lengths,
        slot_block,
        tokens,
        norm_gain,
        parents,
        w_query,
        key_projection,
        value_projection,
        w_out,
        cache_keys,
        paged_value_cache,
    )


def solution(mesh):
    in_specs = (
        P("seq", None),
        P(),
        P(None, "head"),
        P(None, "head"),
        P(None, "head"),
        P("head", None),
        P(None, "seq", "head"),
        P(None, "seq", "head"),
        P(),
        P(),
        P(None, "seq"),
    )
    return jax.shard_map(
        per_device,
        mesh=mesh,
        in_specs=in_specs,
        out_specs=P("seq", "head"),
        check_vma=False,
    )
```

```python
import functools
import math

import jax
import jax.numpy as jnp
from jax import lax
from jax.experimental import pallas as pl
from jax.experimental.pallas import tpu as pltpu
from jax.sharding import PartitionSpec as P

NORM_EPSILON = 1e-05
HIDDEN = -1e30
HEAD_WIDTH = 128
TREE = 64
PAGE = 128
KEY_TILE = 256
WEIGHT_PARTS = 4
ORDER = ((0, 1), (3, 0), (2, 0), (2, 1), (3, 1), (1, 1), (1, 0), (0, 0))
FORWARDS = ((2,), (3, 4), (5,), (6,), (7,), (), (), ())

NT = (((1,), (1,)), ((), ()))
TN = (((0,), (0,)), ((), ()))
F32 = jnp.float32
BF16 = jnp.bfloat16


def layer(
    n_seq,
    n_head,
    lengths_hbm,
    slots_hbm,
    tokens_hbm,
    gain_hbm,
    parents_hbm,
    wq_hbm,
    wk_hbm,
    wv_hbm,
    wo_hbm,
    keys_hbm,
    values_hbm,
    mixed_ref,
    lengths_ref,
    slots_ref,
    tokens_ref,
    gain_ref,
    parents_ref,
    small_sem,
    wqkv,
    wo,
    keys,
    values,
    normed,
    qall,
    kvtree,
    score_a,
    score_b,
    top_a,
    top_b,
    out_own,
    lse_own,
    out_swap,
    lse_swap,
    out_pair,
    lse_pair,
    out_last,
    out_recv,
    lse_recv,
    part_send,
    part_recv,
    w_sem,
    wo_sem,
    cache_sem,
    q_send_sem,
    q_far_sem,
    q_near_sem,
    kv_send_sem,
    kv_recv_sem,
    x_send_sem,
    x_recv_sem,
    xl_send_sem,
    xl_recv_sem,
    o_send_sem,
    o_recv_sem,
    l_send_sem,
    l_recv_sem,
    p_send_sem,
    p_recv_sem,
):
    me = lax.axis_index("seq")
    head = lax.axis_index("head")
    rows, width = tokens_ref.shape
    requests = keys.shape[0]
    context = keys.shape[1]
    owners = TREE // rows
    q_width = wq_hbm.shape[1]
    groups = q_width // HEAD_WIDTH
    block = groups * rows
    queries = owners * block
    tiles = context // KEY_TILE
    own_request = me // owners
    own_place = me % owners
    scale = HEAD_WIDTH**-0.5
    scale2 = scale * math.log2(math.e)

    small = [
        pltpu.make_async_copy(source, target, small_sem.at[n])
        for n, (source, target) in enumerate(
            (
                (tokens_hbm, tokens_ref),
                (gain_hbm, gain_ref),
                (parents_hbm, parents_ref),
                (lengths_hbm, lengths_ref),
                (slots_hbm, slots_ref),
            )
        )
    ]
    for copy in small[:2]:
        copy.start()
    part = width // WEIGHT_PARTS

    wide = 2 * HEAD_WIDTH
    pieces = q_width // wide

    def start_weights(source, first, column, sem):
        for c in range(WEIGHT_PARTS):
            at = pl.ds(c * part, part)
            count = min(wide, source.shape[1])
            pltpu.make_async_copy(
                source.at[at, pl.ds(first, count)],
                wqkv.at[at, pl.ds(column, count)],
                w_sem.at[sem],
            ).start()

    def project(n):
        at = wqkv.at[:, pl.ds(n * wide, wide)]
        pltpu.make_async_copy(at, at, w_sem.at[n]).wait()
        return jnp.dot(
            normed[...],
            wqkv[:, n * wide : (n + 1) * wide],
            preferred_element_type=F32,
        ).astype(BF16)

    own_width = width // n_head

    def wo_copy(j):
        at = pl.ds(pl.multiple_of(j * own_width, own_width), own_width)
        return pltpu.make_async_copy(wo_hbm.at[:, at], wo.at[j], wo_sem)

    core = own_place % 2
    spot = own_place // 2
    chip = me // 2
    partner = me + 1 - 2 * core
    lanes = 128
    chips = n_seq // 2
    chips_x = 2
    joined = requests - 2
    unforwarded = 1

    rows_y = requests // chips_x

    def request_at(i):
        y = own_request // chips_x
        row = (y, y + 1 - 2 * (y % 2), (y + 2) % rows_y, rows_y - 1 - y)[ORDER[i][0]]
        return row * chips_x + (own_request + ORDER[i][1]) % chips_x

    start_weights(wq_hbm, 0, 0, 0)

    barrier = pltpu.get_barrier_semaphore()

    def greet_seq(j, _):
        pl.semaphore_signal(
            barrier,
            inc=1,
            device_id=((me + j) % n_seq, head),
            device_id_type=pl.DeviceIdType.MESH,
        )
        return 0

    def greet_head(j, _):
        pl.semaphore_signal(
            barrier,
            inc=1,
            device_id=(me, (head + j) % n_head),
            device_id_type=pl.DeviceIdType.MESH,
        )
        return 0

    for n in sorted(range(1, n_head), key=lambda d: -min(d, n_head - d)):
        greet_head(n, 0)
    lax.fori_loop(1, n_seq, greet_seq, 0)

    for n in range(1, pieces):
        start_weights(wq_hbm, n * wide, n * wide, n)
    for copy in small[2:]:
        copy.start()

    def start_wo(j, _):
        wo_copy(j).start()
        return 0

    small[0].wait()
    small[1].wait()
    inputs = tokens_ref[...].astype(F32)
    mean = jnp.mean(inputs * inputs, axis=-1, keepdims=True)
    normed[...] = (
        inputs
        * lax.rsqrt(mean + NORM_EPSILON)
        * gain_ref[...].reshape(1, width).astype(F32)
    ).astype(BF16)

    for n in range(pieces):
        projected = project(n)
        if n == 0:
            start_weights(wk_hbm, 0, q_width, pieces)
            start_weights(wv_hbm, 0, q_width + HEAD_WIDTH, pieces)
        for g in range(2):
            line = (n * 2 + g) * rows
            qall[me, line : line + rows, :] = projected[
                :, g * HEAD_WIDTH : (g + 1) * HEAD_WIDTH
            ]

    def remote(source, target, send_sem, recv_sem, peer):
        return pltpu.make_async_remote_copy(
            src_ref=source,
            dst_ref=target,
            send_sem=send_sem,
            recv_sem=recv_sem,
            device_id=(peer, head),
            device_id_type=pl.DeviceIdType.MESH,
        )

    def arrived(ref, count, sem):
        at = pl.ds(0, count)
        pltpu.make_async_copy(ref.at[at], ref.at[at], sem).wait()

    def q_copy(which, recv_sem, peer):
        return remote(qall.at[which], qall.at[which], q_send_sem, recv_sem, peer)

    pl.semaphore_wait(barrier, n_seq - 1 + n_head - 1)

    def q_send(i):
        for n in range(2):
            to = request_at(i) * owners + (spot + n) % 2 * 2
            q_copy(me, q_far_sem.at[own_request], to + core).start()
            if i < unforwarded:
                q_copy(me, q_near_sem.at[own_request], to + 1 - core).start()

    q_send(0)
    q_send(1)
    for i in range(requests):
        r = request_at(i)
        for source, target in ((keys_hbm, keys), (values_hbm, values)):
            pltpu.make_async_copy(source.at[r], target.at[r], cache_sem.at[r]).start()
    lax.fori_loop(0, n_head, start_wo, 0)

    projected = project(pieces)
    for n in range(2):
        kvtree[own_place, n * rows : (n + 1) * rows, :] = projected[
            :, n * HEAD_WIDTH : (n + 1) * HEAD_WIDTH
        ]

    q_send(3)
    q_send(2)

    for copy in small[2:]:
        copy.wait()
    parent = parents_ref[pl.ds(own_request, 1), :]
    node = lax.broadcasted_iota(jnp.int32, (TREE, TREE), 0)
    other = lax.broadcasted_iota(jnp.int32, (TREE, TREE), 1)
    reached = jnp.where((parent == node) | (node == other), 1.0, 0.0)
    for _ in range(max(1, (TREE - 1).bit_length())):
        half = reached.astype(BF16)
        reached = jnp.minimum(jnp.dot(half, half, preferred_element_type=F32), 1.0)

    for n in range(1, owners):
        peer = own_request * owners + (own_place + n) % owners
        mine = kvtree.at[own_place]
        remote(mine, mine, kv_send_sem, kv_recv_sem, peer).start()
    q_send(4)
    q_send(5)

    row_in_page = lax.broadcasted_iota(jnp.int32, (PAGE, queries), 0)

    def forward(i):
        r = request_at(i)
        base = r * owners + core
        if i == requests - 1:
            arrived(qall, 1, q_far_sem.at[r])
            q_copy(beside, q_near_sem.at[r], partner).start()
        else:
            arrived(qall, 2, q_far_sem.at[r])
            q_copy(base, q_near_sem.at[r], partner).start()
            q_copy(base + 2, q_near_sem.at[r], partner).start()

    def wait_for(i):
        r = request_at(i)
        if i < unforwarded:
            arrived(qall, 2, q_far_sem.at[r])
        arrived(qall, 2, q_near_sem.at[r])
        arrived(keys, 2, cache_sem.at[r])

    def score_tile(i, b, best, score):
        r = request_at(i)
        q = qall[pl.ds(r * owners, owners)].reshape(queries, HEAD_WIDTH)
        s = lax.dot_general(
            keys[r, b * KEY_TILE : (b + 1) * KEY_TILE, :],
            q,
            NT,
            preferred_element_type=F32,
        )
        for n in range(KEY_TILE // PAGE):
            p = b * (KEY_TILE // PAGE) + n
            left = lengths_ref[r] - slots_ref[r, p] * PAGE
            shown = jnp.where(
                row_in_page < left, s[n * PAGE : (n + 1) * PAGE], HIDDEN
            )
            score[p * PAGE : (p + 1) * PAGE, :] = shown
            high = jnp.max(shown.reshape(PAGE // 8, 8, queries), axis=0)
            best = high if best is None else jnp.maximum(best, high)
        return best

    def weigh_tile(i, b, state, score, top):
        r = request_at(i)
        acc, total = state
        w = jnp.exp2(score[b * KEY_TILE : (b + 1) * KEY_TILE, :] * scale2 - top)
        low = jnp.sum(w.reshape(KEY_TILE // 8, 8, queries), axis=0)
        added = lax.dot_general(
            values[r, b * KEY_TILE : (b + 1) * KEY_TILE, :],
            w.astype(BF16),
            TN,
            preferred_element_type=F32,
        )
        if acc is None:
            return added, low
        return acc + added, total + low

    def finish(i, state, top, last):
        acc, total = state
        total = jnp.maximum(jnp.sum(total, axis=0, keepdims=True), 1.0)
        out = acc / total
        lse = top * (1.0 / math.log2(math.e)) + jnp.log(total)
        for n in range(2):
            half = slice(n * lanes, (n + 1) * lanes)
            lse_own[i, n] = lse[:, half]
            if not last:
                out_own[i, n] = out[:, half].astype(BF16)
        if last:
            out = out.T.astype(BF16).reshape(owners, block, HEAD_WIDTH)
            out_last[i - joined] = out

    def swap(i):
        other = 1 - core
        remote(
            out_own.at[i, other], out_swap.at[i], x_send_sem, x_recv_sem.at[i], partner
        ).start()
        remote(
            lse_own.at[i, other],
            lse_swap.at[i],
            xl_send_sem,
            xl_recv_sem.at[i],
            partner,
        ).start()

    def wait_swap(i):
        arrived(out_swap, 1, x_recv_sem.at[i])
        arrived(lse_swap, 1, xl_recv_sem.at[i])

    def join(i):
        mine, theirs = lse_own[i, core], lse_swap[i]
        high = jnp.maximum(mine, theirs)
        mine = jnp.exp(mine - high)
        theirs = jnp.exp(theirs - high)
        total = mine + theirs
        out = out_own[i, core].astype(F32) * (mine / total)
        out += out_swap[i].astype(F32) * (theirs / total)
        out_pair[i] = out.T.astype(BF16).reshape(2, block, HEAD_WIDTH)
        lse_pair[i] = high + jnp.log(total)

    def send_pair(i):
        first = request_at(i) * owners + core * 2

        for n in range(2):
            place = (core + n) % 2
            peer = first + place
            remote(
                out_pair.at[i, place], out_recv.at[chip], o_send_sem, o_recv_sem, peer
            ).start()
            remote(
                lse_pair.at[i], lse_recv.at[chip], l_send_sem, l_recv_sem, peer
            ).start()

    def send_direct(i):
        r = request_at(i)
        own = i == requests - 1
        spare = chips + (i - joined) * 2 + chip % 2
        slot = chip * (1 - core) + spare * core

        def send(n, _):
            place = (own_place + n) % owners
            peer = r * owners + place
            remote(
                out_last.at[i - joined, place],
                out_recv.at[slot],
                o_send_sem,
                o_recv_sem,
                peer,
            ).start()
            remote(
                lse_own.at[i, place // 2],
                lse_recv.at[slot],
                l_send_sem,
                l_recv_sem,
                peer,
            ).start()
            return 0

        lax.fori_loop(1 if own else 0, owners, send, 0)
        if own:
            out_recv[slot] = out_last[i - joined, own_place]
            lse_recv[slot] = lse_own[i, spot]

    def half_step(i, now, after):
        joins = 2 <= i < requests - 1
        direct = i >= joined
        for n in FORWARDS[i]:
            forward(n)
        if after is not None:
            wait_for(i + 1)
        if joins:
            wait_swap(i - 2)
        score, top_ref = now
        top = jnp.max(top_ref[...], axis=0, keepdims=True) * scale2
        state = (None, None)
        best = None
        for b in range(tiles):
            if after is not None:
                best = score_tile(i + 1, b, best, after[0])
            state = weigh_tile(i, b, state, score, top)
        if after is not None:
            after[1][...] = best
        finish(i, state, top, direct)
        if joins:
            join(i - 2)
        if direct:
            send_direct(i)
        else:
            swap(i)
        if joins:
            send_pair(i - 2)
        if i == joined:
            wait_swap(i - 1)
            join(i - 1)
            send_pair(i - 1)

    a, b = (score_a, top_a), (score_b, top_b)
    wait_for(0)
    forward(1)
    best = None
    for t in range(tiles):
        best = score_tile(0, t, best, score_a)
    top_a[...] = best
    q_send(6)
    q_copy(me, q_near_sem.at[own_request], partner).start()
    beside = own_request * owners + (1 - spot) * 2 + core
    q_copy(me, q_far_sem.at[own_request], beside).start()
    for n in range(requests // 2):
        for i, now, after in ((2 * n, a, b), (2 * n + 1, b, a)):
            half_step(i, now, after if i < requests - 1 else None)

    arrived(kvtree, owners - 1, kv_recv_sem)
    own_queries = qall[me]
    own_queries = jnp.concatenate([own_queries] * (lanes // block), axis=0)
    tree_keys = kvtree[:, :rows, :].reshape(TREE, HEAD_WIDTH)
    tree_values = kvtree[:, rows:, :].reshape(TREE, HEAD_WIDTH)
    token = lax.broadcasted_iota(jnp.int32, (TREE, lanes), 0)
    lane = lax.broadcasted_iota(jnp.int32, (TREE, lanes), 1)
    pick = jnp.where(token == own_place * rows + lane % rows, 1.0, 0.0).astype(BF16)
    seen = jnp.dot(reached.astype(BF16), pick, preferred_element_type=F32) > 0.5
    tree_scores = lax.dot_general(
        tree_keys, own_queries, NT, preferred_element_type=F32
    )
    tree_scores = jnp.where(seen, tree_scores, HIDDEN)
    tree_top = jnp.max(tree_scores, axis=0, keepdims=True)
    tree_weights = jnp.where(
        seen, jnp.exp2(tree_scores * scale2 - tree_top * scale2), 0.0
    )
    tree_total = jnp.maximum(jnp.sum(tree_weights, axis=0, keepdims=True), 1.0)
    tree_sum = lax.dot_general(
        tree_values, tree_weights.astype(BF16), TN, preferred_element_type=F32
    )
    blocks = chips + 2 * (requests - joined)
    out_recv[blocks] = (tree_sum / tree_total).T[:block].astype(BF16)
    lse_recv[blocks] = tree_top * scale + jnp.log(tree_total)
    for n in range(blocks + 1, lse_recv.shape[0]):
        lse_recv[n] = jnp.full((1, lanes), HIDDEN, F32)
    arrived(wo, n_head, wo_sem)

    arrived(lse_recv, blocks - 1, l_recv_sem)
    lse = lse_recv[...].reshape(lse_recv.shape[0], lanes)
    lse = pltpu.roll(lse, (lanes - core * block) % lanes, 1)
    factor = jnp.exp(lse - jnp.max(lse, axis=0, keepdims=True))
    factor = (factor / jnp.sum(factor, axis=0, keepdims=True)).T[:block]
    arrived(out_recv, blocks - 1, o_recv_sem)
    merged = jnp.zeros((block, HEAD_WIDTH), F32)
    for n in range(blocks + 1):
        merged += out_recv[n].astype(F32) * factor[:, n : n + 1]
    merged = merged.astype(BF16)
    attended = jnp.concatenate(
        [merged[g * rows : (g + 1) * rows] for g in range(groups)], axis=1
    )

    def piece(j):
        return jnp.dot(attended, wo[j], preferred_element_type=F32)

    def part_copy(j):
        return pltpu.make_async_remote_copy(
            src_ref=part_send.at[j],
            dst_ref=part_recv.at[head],
            send_sem=p_send_sem,
            recv_sem=p_recv_sem,
            device_id=(me, j),
            device_id_type=pl.DeviceIdType.MESH,
        )

    order = sorted(range(1, n_head), key=lambda d: -min(d, n_head - d))
    for d in order:
        j = (head + d) % n_head
        part_send[j] = piece(j).astype(BF16)
        part_copy(j).start()
    mine = piece(head)
    at = pl.ds(pl.multiple_of(head * own_width, own_width), own_width)
    mine = mine + tokens_ref[:, at].astype(F32)
    part_recv[head] = jnp.zeros((rows, own_width), BF16)
    arrived(part_recv, n_head - 1, p_recv_sem)
    mixed_ref[...] = (mine + jnp.sum(part_recv[...].astype(F32), axis=0)).astype(BF16)

    arrived(part_send, n_head - 1, p_send_sem)
    arrived(qall, n_seq - 1, q_send_sem)
    arrived(kvtree, owners - 1, kv_send_sem)
    arrived(out_swap, joined, x_send_sem)
    arrived(lse_swap, joined, xl_send_sem)
    arrived(out_recv, blocks - 1, o_send_sem)
    arrived(lse_recv, blocks - 1, l_send_sem)


def per_device(
    tokens,
    norm_gain,
    w_query,
    key_projection,
    value_projection,
    w_out,
    cache_keys,
    paged_value_cache,
    lengths,
    parents,
    slot_block,
):
    n_seq = lax.axis_size("seq")
    n_head = lax.axis_size("head")
    rows, width = tokens.shape
    requests, context, _ = cache_keys.shape
    q_width = w_query.shape[1]
    groups = q_width // HEAD_WIDTH
    owners = TREE // rows
    block = groups * rows
    queries = owners * block
    own_width = width // n_head
    vmem = pl.BlockSpec(memory_space=pltpu.VMEM)
    hbm = pl.BlockSpec(memory_space=pltpu.HBM)
    dma = pltpu.SemaphoreType.DMA
    return pl.pallas_call(
        functools.partial(layer, n_seq, n_head),
        out_shape=pltpu.VMEM((rows, own_width), BF16),
        in_specs=[hbm] * 11,
        out_specs=vmem,
        scratch_shapes=[
            pltpu.SMEM(lengths.shape, jnp.int32),
            pltpu.SMEM(slot_block.shape, jnp.int32),
            pltpu.VMEM(tokens.shape, BF16),
            pltpu.VMEM(norm_gain.shape, BF16),
            pltpu.VMEM(parents.shape, jnp.int32),
            dma((5,)),
            pltpu.VMEM((width, q_width + 2 * HEAD_WIDTH), BF16),
            pltpu.VMEM((n_head, q_width, own_width), BF16),
            pltpu.VMEM((requests, context, HEAD_WIDTH), BF16),
            pltpu.VMEM((requests, context, HEAD_WIDTH), BF16),
            pltpu.VMEM((rows, width), BF16),
            pltpu.VMEM((n_seq, block, HEAD_WIDTH), BF16),
            pltpu.VMEM((owners, 2 * rows, HEAD_WIDTH), BF16),
            pltpu.VMEM((context, queries), F32),
            pltpu.VMEM((context, queries), F32),
            pltpu.VMEM((8, queries), F32),
            pltpu.VMEM((8, queries), F32),
            pltpu.VMEM((requests, 2, HEAD_WIDTH, 2 * block), BF16),
            pltpu.VMEM((requests, 2, 1, 2 * block), F32),
            pltpu.VMEM((requests, HEAD_WIDTH, 2 * block), BF16),
            pltpu.VMEM((requests, 1, 2 * block), F32),
            pltpu.VMEM((requests, 2, block, HEAD_WIDTH), BF16),
            pltpu.VMEM((requests, 1, 2 * block), F32),
            pltpu.VMEM((2, owners, block, HEAD_WIDTH), BF16),
            pltpu.VMEM((24, block, HEAD_WIDTH), BF16),
            pltpu.VMEM((24, 1, 2 * block), F32),
            pltpu.VMEM((n_head, rows, own_width), BF16),
            pltpu.VMEM((n_head, rows, own_width), BF16),
            dma((q_width // (2 * HEAD_WIDTH) + 1,)),
            dma,
            dma((requests,)),
            dma,
            dma((requests,)),
            dma((requests,)),
            dma,
            dma,
            dma,
            dma((requests - 2,)),
            dma,
            dma((requests - 2,)),
            dma,
            dma,
            dma,
            dma,
            dma,
            dma,
        ],
        compiler_params=pltpu.CompilerParams(
            collective_id=0,
            has_side_effects=True,
            vmem_limit_bytes=60 * 1024 * 1024,
        ),
        name="layer",
    )(
        lengths,
        slot_block,
        tokens,
        norm_gain,
        parents,
        w_query,
        key_projection,
        value_projection,
        w_out,
        cache_keys,
        paged_value_cache,
    )


def solution(mesh):
    in_specs = (
        P("seq", None),
        P(),
        P(None, "head"),
        P(None, "head"),
        P(None, "head"),
        P("head", None),
        P(None, "seq", "head"),
        P(None, "seq", "head"),
        P(),
        P(),
        P(None, "seq"),
    )
    return jax.shard_map(
        per_device,
        mesh=mesh,
        in_specs=in_specs,
        out_specs=P("seq", "head"),
        check_vma=False,
    )
```

```python
import functools
import math

import jax
import jax.numpy as jnp
from jax import lax
from jax.experimental import pallas as pl
from jax.experimental.pallas import tpu as pltpu
from jax.sharding import PartitionSpec as P

NORM_EPSILON = 1e-05
HIDDEN = -1e30
HEAD_WIDTH = 128
TREE = 64
PAGE = 128
KEY_TILE = 256
SCORE_TILE = 512
WEIGHT_PARTS = 4
ORDER = ((0, 1), (3, 0), (2, 0), (2, 1), (3, 1), (1, 1), (1, 0), (0, 0))
FORWARDS = ((2,), (3, 4), (5,), (6,), (7,), (), (), ())

NT = (((1,), (1,)), ((), ()))
TN = (((0,), (0,)), ((), ()))
F32 = jnp.float32
BF16 = jnp.bfloat16


def layer(
    n_seq,
    n_head,
    lengths_hbm,
    slots_hbm,
    tokens_hbm,
    gain_hbm,
    parents_hbm,
    wq_hbm,
    wk_hbm,
    wv_hbm,
    wo_hbm,
    keys_hbm,
    values_hbm,
    mixed_ref,
    lengths_ref,
    slots_ref,
    tokens_ref,
    gain_ref,
    parents_ref,
    small_sem,
    wqkv,
    wo,
    keys,
    values,
    normed,
    qall,
    kvtree,
    score_a,
    score_b,
    top_a,
    top_b,
    out_own,
    lse_own,
    out_swap,
    lse_swap,
    out_pair,
    lse_pair,
    out_last,
    out_recv,
    lse_recv,
    part_send,
    part_recv,
    w_sem,
    wo_sem,
    cache_sem,
    q_send_sem,
    q_far_sem,
    q_near_sem,
    kv_send_sem,
    kv_recv_sem,
    x_send_sem,
    x_recv_sem,
    xl_send_sem,
    xl_recv_sem,
    o_send_sem,
    o_recv_sem,
    l_send_sem,
    l_recv_sem,
    p_send_sem,
    p_recv_sem,
):
    me = lax.axis_index("seq")
    head = lax.axis_index("head")
    rows, width = tokens_ref.shape
    requests = keys.shape[0]
    context = keys.shape[1]
    owners = TREE // rows
    q_width = wq_hbm.shape[1]
    groups = q_width // HEAD_WIDTH
    block = groups * rows
    queries = owners * block
    tiles = context // KEY_TILE
    every = SCORE_TILE // KEY_TILE
    own_request = me // owners
    own_place = me % owners
    scale = HEAD_WIDTH**-0.5
    scale2 = scale * math.log2(math.e)

    small = [
        pltpu.make_async_copy(source, target, small_sem.at[n])
        for n, (source, target) in enumerate(
            (
                (tokens_hbm, tokens_ref),
                (gain_hbm, gain_ref),
                (parents_hbm, parents_ref),
                (lengths_hbm, lengths_ref),
                (slots_hbm, slots_ref),
            )
        )
    ]
    for copy in small[:2]:
        copy.start()
    part = width // WEIGHT_PARTS

    wide = 2 * HEAD_WIDTH
    pieces = q_width // wide

    def start_weights(source, first, column, sem):
        for c in range(WEIGHT_PARTS):
            at = pl.ds(c * part, part)
            count = min(wide, source.shape[1])
            pltpu.make_async_copy(
                source.at[at, pl.ds(first, count)],
                wqkv.at[at, pl.ds(column, count)],
                w_sem.at[sem],
            ).start()

    def project(n):
        at = wqkv.at[:, pl.ds(n * wide, wide)]
        pltpu.make_async_copy(at, at, w_sem.at[n]).wait()
        return jnp.dot(
            normed[...],
            wqkv[:, n * wide : (n + 1) * wide],
            preferred_element_type=F32,
        ).astype(BF16)

    own_width = width // n_head

    def wo_copy(j):
        at = pl.ds(pl.multiple_of(j * own_width, own_width), own_width)
        return pltpu.make_async_copy(wo_hbm.at[:, at], wo.at[j], wo_sem)

    core = own_place % 2
    spot = own_place // 2
    chip = me // 2
    partner = me + 1 - 2 * core
    lanes = 128
    chips = n_seq // 2
    chips_x = 2
    joined = requests - 2
    unforwarded = 1

    rows_y = requests // chips_x

    def request_at(i):
        y = own_request // chips_x
        row = (y, y + 1 - 2 * (y % 2), (y + 2) % rows_y, rows_y - 1 - y)[ORDER[i][0]]
        return row * chips_x + (own_request + ORDER[i][1]) % chips_x

    start_weights(wq_hbm, 0, 0, 0)

    barrier = pltpu.get_barrier_semaphore()

    def greet_seq(j, _):
        pl.semaphore_signal(
            barrier,
            inc=1,
            device_id=((me + j) % n_seq, head),
            device_id_type=pl.DeviceIdType.MESH,
        )
        return 0

    def greet_head(j, _):
        pl.semaphore_signal(
            barrier,
            inc=1,
            device_id=(me, (head + j) % n_head),
            device_id_type=pl.DeviceIdType.MESH,
        )
        return 0

    for n in sorted(range(1, n_head), key=lambda d: -min(d, n_head - d)):
        greet_head(n, 0)
    lax.fori_loop(1, n_seq, greet_seq, 0)

    for n in range(1, pieces):
        start_weights(wq_hbm, n * wide, n * wide, n)
    for copy in small[2:]:
        copy.start()

    def start_wo(j, _):
        wo_copy(j).start()
        return 0

    small[0].wait()
    small[1].wait()
    inputs = tokens_ref[...].astype(F32)
    mean = jnp.mean(inputs * inputs, axis=-1, keepdims=True)
    normed[...] = (
        inputs
        * lax.rsqrt(mean + NORM_EPSILON)
        * gain_ref[...].reshape(1, width).astype(F32)
    ).astype(BF16)

    for n in range(pieces):
        projected = project(n)
        if n == 0:
            start_weights(wk_hbm, 0, q_width, pieces)
            start_weights(wv_hbm, 0, q_width + HEAD_WIDTH, pieces)
        for g in range(2):
            line = (n * 2 + g) * rows
            qall[me, line : line + rows, :] = projected[
                :, g * HEAD_WIDTH : (g + 1) * HEAD_WIDTH
            ]

    def remote(source, target, send_sem, recv_sem, peer):
        return pltpu.make_async_remote_copy(
            src_ref=source,
            dst_ref=target,
            send_sem=send_sem,
            recv_sem=recv_sem,
            device_id=(peer, head),
            device_id_type=pl.DeviceIdType.MESH,
        )

    def arrived(ref, count, sem):
        at = pl.ds(0, count)
        pltpu.make_async_copy(ref.at[at], ref.at[at], sem).wait()

    def q_copy(which, recv_sem, peer):
        return remote(qall.at[which], qall.at[which], q_send_sem, recv_sem, peer)

    pl.semaphore_wait(barrier, n_seq - 1 + n_head - 1)

    def q_send(i):
        for n in range(2):
            to = request_at(i) * owners + (spot + n) % 2 * 2
            q_copy(me, q_far_sem.at[own_request], to + core).start()
            if i < unforwarded:
                q_copy(me, q_near_sem.at[own_request], to + 1 - core).start()

    q_send(0)
    q_send(1)
    for i in range(requests):
        r = request_at(i)
        for source, target in ((keys_hbm, keys), (values_hbm, values)):
            pltpu.make_async_copy(source.at[r], target.at[r], cache_sem.at[r]).start()
    lax.fori_loop(0, n_head, start_wo, 0)

    projected = project(pieces)
    for n in range(2):
        kvtree[own_place, n * rows : (n + 1) * rows, :] = projected[
            :, n * HEAD_WIDTH : (n + 1) * HEAD_WIDTH
        ]

    q_send(3)
    q_send(2)

    for copy in small[2:]:
        copy.wait()
    parent = parents_ref[pl.ds(own_request, 1), :]
    node = lax.broadcasted_iota(jnp.int32, (TREE, TREE), 0)
    other = lax.broadcasted_iota(jnp.int32, (TREE, TREE), 1)
    reached = jnp.where((parent == node) | (node == other), 1.0, 0.0)
    for _ in range(max(1, (TREE - 1).bit_length())):
        half = reached.astype(BF16)
        reached = jnp.minimum(jnp.dot(half, half, preferred_element_type=F32), 1.0)

    for n in range(1, owners):
        peer = own_request * owners + (own_place + n) % owners
        mine = kvtree.at[own_place]
        remote(mine, mine, kv_send_sem, kv_recv_sem, peer).start()
    q_send(4)
    q_send(5)

    row_in_page = lax.broadcasted_iota(jnp.int32, (PAGE, queries), 0)

    def forward(i):
        r = request_at(i)
        base = r * owners + core
        if i == requests - 1:
            arrived(qall, 1, q_far_sem.at[r])
            q_copy(beside, q_near_sem.at[r], partner).start()
        else:
            arrived(qall, 2, q_far_sem.at[r])
            q_copy(base, q_near_sem.at[r], partner).start()
            q_copy(base + 2, q_near_sem.at[r], partner).start()

    def wait_for(i):
        r = request_at(i)
        if i < unforwarded:
            arrived(qall, 2, q_far_sem.at[r])
        arrived(qall, 2, q_near_sem.at[r])
        arrived(keys, 2, cache_sem.at[r])

    def score_tile(i, b, best, score):
        r = request_at(i)
        q = qall[pl.ds(r * owners, owners)].reshape(queries, HEAD_WIDTH)
        s = lax.dot_general(
            keys[r, b * SCORE_TILE : (b + 1) * SCORE_TILE, :],
            q,
            NT,
            preferred_element_type=F32,
        )
        for n in range(SCORE_TILE // PAGE):
            p = b * (SCORE_TILE // PAGE) + n
            left = lengths_ref[r] - slots_ref[r, p] * PAGE
            shown = jnp.where(
                row_in_page < left, s[n * PAGE : (n + 1) * PAGE], HIDDEN
            )
            score[p * PAGE : (p + 1) * PAGE, :] = shown
            high = jnp.max(shown.reshape(PAGE // 8, 8, queries), axis=0)
            best = high if best is None else jnp.maximum(best, high)
        return best

    def weigh_tile(i, b, state, score, top):
        r = request_at(i)
        acc, total = state
        w = jnp.exp2(score[b * KEY_TILE : (b + 1) * KEY_TILE, :] * scale2 - top)
        low = jnp.sum(w.reshape(KEY_TILE // 8, 8, queries), axis=0)
        added = lax.dot_general(
            values[r, b * KEY_TILE : (b + 1) * KEY_TILE, :],
            w.astype(BF16),
            TN,
            preferred_element_type=F32,
        )
        if acc is None:
            return added, low
        return acc + added, total + low

    def finish(i, state, top, last):
        acc, total = state
        total = jnp.maximum(jnp.sum(total, axis=0, keepdims=True), 1.0)
        out = acc / total
        lse = top * (1.0 / math.log2(math.e)) + jnp.log(total)
        for n in range(2):
            half = slice(n * lanes, (n + 1) * lanes)
            lse_own[i, n] = lse[:, half]
            if not last:
                out_own[i, n] = out[:, half].astype(BF16)
        if last:
            out = out.T.astype(BF16).reshape(owners, block, HEAD_WIDTH)
            out_last[i - joined] = out

    def swap(i):
        other = 1 - core
        remote(
            out_own.at[i, other], out_swap.at[i], x_send_sem, x_recv_sem.at[i], partner
        ).start()
        remote(
            lse_own.at[i, other],
            lse_swap.at[i],
            xl_send_sem,
            xl_recv_sem.at[i],
            partner,
        ).start()

    def wait_swap(i):
        arrived(out_swap, 1, x_recv_sem.at[i])
        arrived(lse_swap, 1, xl_recv_sem.at[i])

    def join(i):
        mine, theirs = lse_own[i, core], lse_swap[i]
        high = jnp.maximum(mine, theirs)
        mine = jnp.exp(mine - high)
        theirs = jnp.exp(theirs - high)
        total = mine + theirs
        out = out_own[i, core].astype(F32) * (mine / total)
        out += out_swap[i].astype(F32) * (theirs / total)
        out_pair[i] = out.T.astype(BF16).reshape(2, block, HEAD_WIDTH)
        lse_pair[i] = high + jnp.log(total)

    def send_pair(i):
        first = request_at(i) * owners + core * 2

        for n in range(2):
            place = (core + n) % 2
            peer = first + place
            remote(
                out_pair.at[i, place], out_recv.at[chip], o_send_sem, o_recv_sem, peer
            ).start()
            remote(
                lse_pair.at[i], lse_recv.at[chip], l_send_sem, l_recv_sem, peer
            ).start()

    def send_direct(i):
        r = request_at(i)
        own = i == requests - 1
        spare = chips + (i - joined) * 2 + chip % 2
        slot = chip * (1 - core) + spare * core

        def send(n, _):
            place = (own_place + n) % owners
            peer = r * owners + place
            remote(
                out_last.at[i - joined, place],
                out_recv.at[slot],
                o_send_sem,
                o_recv_sem,
                peer,
            ).start()
            remote(
                lse_own.at[i, place // 2],
                lse_recv.at[slot],
                l_send_sem,
                l_recv_sem,
                peer,
            ).start()
            return 0

        lax.fori_loop(1 if own else 0, owners, send, 0)
        if own:
            out_recv[slot] = out_last[i - joined, own_place]
            lse_recv[slot] = lse_own[i, spot]

    def half_step(i, now, after):
        joins = 2 <= i < requests - 1
        direct = i >= joined
        for n in FORWARDS[i]:
            forward(n)
        if after is not None:
            wait_for(i + 1)
        if joins:
            wait_swap(i - 2)
        score, top_ref = now
        top = jnp.max(top_ref[...], axis=0, keepdims=True) * scale2
        state = (None, None)
        best = None
        for b in range(tiles):
            state = weigh_tile(i, b, state, score, top)
            if after is not None and b % every == 0:
                best = score_tile(i + 1, b // every, best, after[0])
        if after is not None:
            after[1][...] = best
        finish(i, state, top, direct)
        if joins:
            join(i - 2)
        if direct:
            send_direct(i)
        else:
            swap(i)
        if joins:
            send_pair(i - 2)
        if i == joined:
            wait_swap(i - 1)
            join(i - 1)
            send_pair(i - 1)

    a, b = (score_a, top_a), (score_b, top_b)
    wait_for(0)
    forward(1)
    best = None
    for t in range(tiles // every):
        best = score_tile(0, t, best, score_a)
    top_a[...] = best
    q_send(6)
    q_copy(me, q_near_sem.at[own_request], partner).start()
    beside = own_request * owners + (1 - spot) * 2 + core
    q_copy(me, q_far_sem.at[own_request], beside).start()
    for n in range(requests // 2):
        for i, now, after in ((2 * n, a, b), (2 * n + 1, b, a)):
            half_step(i, now, after if i < requests - 1 else None)

    arrived(kvtree, owners - 1, kv_recv_sem)
    own_queries = qall[me]
    own_queries = jnp.concatenate([own_queries] * (lanes // block), axis=0)
    tree_keys = kvtree[:, :rows, :].reshape(TREE, HEAD_WIDTH)
    tree_values = kvtree[:, rows:, :].reshape(TREE, HEAD_WIDTH)
    token = lax.broadcasted_iota(jnp.int32, (TREE, lanes), 0)
    lane = lax.broadcasted_iota(jnp.int32, (TREE, lanes), 1)
    pick = jnp.where(token == own_place * rows + lane % rows, 1.0, 0.0).astype(BF16)
    seen = jnp.dot(reached.astype(BF16), pick, preferred_element_type=F32) > 0.5
    tree_scores = lax.dot_general(
        tree_keys, own_queries, NT, preferred_element_type=F32
    )
    tree_scores = jnp.where(seen, tree_scores, HIDDEN)
    tree_top = jnp.max(tree_scores, axis=0, keepdims=True)
    tree_weights = jnp.where(
        seen, jnp.exp2(tree_scores * scale2 - tree_top * scale2), 0.0
    )
    tree_total = jnp.maximum(jnp.sum(tree_weights, axis=0, keepdims=True), 1.0)
    tree_sum = lax.dot_general(
        tree_values, tree_weights.astype(BF16), TN, preferred_element_type=F32
    )
    blocks = chips + 2 * (requests - joined)
    out_recv[blocks] = (tree_sum / tree_total).T[:block].astype(BF16)
    lse_recv[blocks] = tree_top * scale + jnp.log(tree_total)
    for n in range(blocks + 1, lse_recv.shape[0]):
        lse_recv[n] = jnp.full((1, lanes), HIDDEN, F32)
    arrived(wo, n_head, wo_sem)

    arrived(lse_recv, blocks - 1, l_recv_sem)
    lse = lse_recv[...].reshape(lse_recv.shape[0], lanes)
    lse = pltpu.roll(lse, (lanes - core * block) % lanes, 1)
    factor = jnp.exp(lse - jnp.max(lse, axis=0, keepdims=True))
    factor = (factor / jnp.sum(factor, axis=0, keepdims=True)).T[:block]
    arrived(out_recv, blocks - 1, o_recv_sem)
    merged = jnp.zeros((block, HEAD_WIDTH), F32)
    for n in range(blocks + 1):
        merged += out_recv[n].astype(F32) * factor[:, n : n + 1]
    merged = merged.astype(BF16)
    attended = jnp.concatenate(
        [merged[g * rows : (g + 1) * rows] for g in range(groups)], axis=1
    )

    def piece(j):
        return jnp.dot(attended, wo[j], preferred_element_type=F32)

    def part_copy(j):
        return pltpu.make_async_remote_copy(
            src_ref=part_send.at[j],
            dst_ref=part_recv.at[head],
            send_sem=p_send_sem,
            recv_sem=p_recv_sem,
            device_id=(me, j),
            device_id_type=pl.DeviceIdType.MESH,
        )

    order = sorted(range(1, n_head), key=lambda d: -min(d, n_head - d))
    for d in order:
        j = (head + d) % n_head
        part_send[j] = piece(j).astype(BF16)
        part_copy(j).start()
    mine = piece(head)
    at = pl.ds(pl.multiple_of(head * own_width, own_width), own_width)
    mine = mine + tokens_ref[:, at].astype(F32)
    part_recv[head] = jnp.zeros((rows, own_width), BF16)
    arrived(part_recv, n_head - 1, p_recv_sem)
    mixed_ref[...] = (mine + jnp.sum(part_recv[...].astype(F32), axis=0)).astype(BF16)

    arrived(part_send, n_head - 1, p_send_sem)
    arrived(qall, n_seq - 1, q_send_sem)
    arrived(kvtree, owners - 1, kv_send_sem)
    arrived(out_swap, joined, x_send_sem)
    arrived(lse_swap, joined, xl_send_sem)
    arrived(out_recv, blocks - 1, o_send_sem)
    arrived(lse_recv, blocks - 1, l_send_sem)


def per_device(
    tokens,
    norm_gain,
    w_query,
    key_projection,
    value_projection,
    w_out,
    cache_keys,
    paged_value_cache,
    lengths,
    parents,
    slot_block,
):
    n_seq = lax.axis_size("seq")
    n_head = lax.axis_size("head")
    rows, width = tokens.shape
    requests, context, _ = cache_keys.shape
    q_width = w_query.shape[1]
    groups = q_width // HEAD_WIDTH
    owners = TREE // rows
    block = groups * rows
    queries = owners * block
    own_width = width // n_head
    vmem = pl.BlockSpec(memory_space=pltpu.VMEM)
    hbm = pl.BlockSpec(memory_space=pltpu.HBM)
    dma = pltpu.SemaphoreType.DMA
    return pl.pallas_call(
        functools.partial(layer, n_seq, n_head),
        out_shape=pltpu.VMEM((rows, own_width), BF16),
        in_specs=[hbm] * 11,
        out_specs=vmem,
        scratch_shapes=[
            pltpu.SMEM(lengths.shape, jnp.int32),
            pltpu.SMEM(slot_block.shape, jnp.int32),
            pltpu.VMEM(tokens.shape, BF16),
            pltpu.VMEM(norm_gain.shape, BF16),
            pltpu.VMEM(parents.shape, jnp.int32),
            dma((5,)),
            pltpu.VMEM((width, q_width + 2 * HEAD_WIDTH), BF16),
            pltpu.VMEM((n_head, q_width, own_width), BF16),
            pltpu.VMEM((requests, context, HEAD_WIDTH), BF16),
            pltpu.VMEM((requests, context, HEAD_WIDTH), BF16),
            pltpu.VMEM((rows, width), BF16),
            pltpu.VMEM((n_seq, block, HEAD_WIDTH), BF16),
            pltpu.VMEM((owners, 2 * rows, HEAD_WIDTH), BF16),
            pltpu.VMEM((context, queries), F32),
            pltpu.VMEM((context, queries), F32),
            pltpu.VMEM((8, queries), F32),
            pltpu.VMEM((8, queries), F32),
            pltpu.VMEM((requests, 2, HEAD_WIDTH, 2 * block), BF16),
            pltpu.VMEM((requests, 2, 1, 2 * block), F32),
            pltpu.VMEM((requests, HEAD_WIDTH, 2 * block), BF16),
            pltpu.VMEM((requests, 1, 2 * block), F32),
            pltpu.VMEM((requests, 2, block, HEAD_WIDTH), BF16),
            pltpu.VMEM((requests, 1, 2 * block), F32),
            pltpu.VMEM((2, owners, block, HEAD_WIDTH), BF16),
            pltpu.VMEM((24, block, HEAD_WIDTH), BF16),
            pltpu.VMEM((24, 1, 2 * block), F32),
            pltpu.VMEM((n_head, rows, own_width), BF16),
            pltpu.VMEM((n_head, rows, own_width), BF16),
            dma((q_width // (2 * HEAD_WIDTH) + 1,)),
            dma,
            dma((requests,)),
            dma,
            dma((requests,)),
            dma((requests,)),
            dma,
            dma,
            dma,
            dma((requests - 2,)),
            dma,
            dma((requests - 2,)),
            dma,
            dma,
            dma,
            dma,
            dma,
            dma,
        ],
        compiler_params=pltpu.CompilerParams(
            collective_id=0,
            has_side_effects=True,
            vmem_limit_bytes=60 * 1024 * 1024,
        ),
        name="layer",
    )(
        lengths,
        slot_block,
        tokens,
        norm_gain,
        parents,
        w_query,
        key_projection,
        value_projection,
        w_out,
        cache_keys,
        paged_value_cache,
    )


def solution(mesh):
    in_specs = (
        P("seq", None),
        P(),
        P(None, "head"),
        P(None, "head"),
        P(None, "head"),
        P("head", None),
        P(None, "seq", "head"),
        P(None, "seq", "head"),
        P(),
        P(),
        P(None, "seq"),
    )
    return jax.shard_map(
        per_device,
        mesh=mesh,
        in_specs=in_specs,
        out_specs=P("seq", "head"),
        check_vma=False,
    )
```

```python
import functools
import math

import jax
import jax.numpy as jnp
from jax import lax
from jax.experimental import pallas as pl
from jax.experimental.pallas import tpu as pltpu
from jax.sharding import PartitionSpec as P

NORM_EPSILON = 1e-05
HIDDEN = -1e30
HEAD_WIDTH = 128
TREE = 64
PAGE = 128
KEY_TILE = 256
SCORE_TILE = 512
WEIGHT_PARTS = 4
ORDER = ((0, 1), (3, 0), (2, 0), (2, 1), (3, 1), (1, 1), (1, 0), (0, 0))
FORWARDS = ((2,), (3, 4), (5,), (6,), (7,), (), (), ())

NT = (((1,), (1,)), ((), ()))
TN = (((0,), (0,)), ((), ()))
F32 = jnp.float32
BF16 = jnp.bfloat16


def layer(
    n_seq,
    n_head,
    lengths_hbm,
    slots_hbm,
    tokens_hbm,
    gain_hbm,
    parents_hbm,
    wq_hbm,
    wk_hbm,
    wv_hbm,
    wo_hbm,
    keys_hbm,
    values_hbm,
    mixed_ref,
    lengths_ref,
    slots_ref,
    tokens_ref,
    gain_ref,
    parents_ref,
    small_sem,
    wqkv,
    wo,
    keys,
    values,
    normed,
    qall,
    kvtree,
    score_a,
    score_b,
    top_a,
    top_b,
    out_own,
    lse_own,
    out_swap,
    lse_swap,
    out_pair,
    lse_pair,
    out_last,
    out_recv,
    lse_recv,
    part_send,
    part_recv,
    w_sem,
    wo_sem,
    cache_sem,
    q_send_sem,
    q_far_sem,
    q_near_sem,
    kv_send_sem,
    kv_recv_sem,
    x_send_sem,
    x_recv_sem,
    xl_send_sem,
    xl_recv_sem,
    o_send_sem,
    o_recv_sem,
    l_send_sem,
    l_recv_sem,
    p_send_sem,
    p_recv_sem,
):
    me = lax.axis_index("seq")
    head = lax.axis_index("head")
    rows, width = tokens_ref.shape
    requests = keys.shape[0]
    context = keys.shape[1]
    owners = TREE // rows
    q_width = wq_hbm.shape[1]
    groups = q_width // HEAD_WIDTH
    block = groups * rows
    queries = owners * block
    tiles = context // KEY_TILE
    every = SCORE_TILE // KEY_TILE
    own_request = me // owners
    own_place = me % owners
    scale = HEAD_WIDTH**-0.5
    scale2 = scale * math.log2(math.e)

    small = [
        pltpu.make_async_copy(source, target, small_sem.at[n])
        for n, (source, target) in enumerate(
            (
                (tokens_hbm, tokens_ref),
                (gain_hbm, gain_ref),
                (parents_hbm, parents_ref),
                (lengths_hbm, lengths_ref),
                (slots_hbm, slots_ref),
            )
        )
    ]
    for copy in small[:2]:
        copy.start()
    part = width // WEIGHT_PARTS

    wide = 2 * HEAD_WIDTH
    pieces = q_width // wide

    halves = 2
    deep = width // halves

    def start_weights(source, first, column, sem):
        for c in range(WEIGHT_PARTS):
            at = pl.ds(c * part, part)
            count = min(wide, source.shape[1])
            pltpu.make_async_copy(
                source.at[at, pl.ds(first, count)],
                wqkv.at[at, pl.ds(column, count)],
                w_sem.at[sem, c * halves // WEIGHT_PARTS],
            ).start()

    def project(n):
        total = None
        for h in range(halves):
            at = wqkv.at[pl.ds(h * deep, deep), pl.ds(n * wide, wide)]
            pltpu.make_async_copy(at, at, w_sem.at[n, h]).wait()
            added = jnp.dot(
                normed[:, h * deep : (h + 1) * deep],
                wqkv[h * deep : (h + 1) * deep, n * wide : (n + 1) * wide],
                preferred_element_type=F32,
            )
            total = added if total is None else total + added
        return total.astype(BF16)

    own_width = width // n_head

    def wo_copy(j):
        at = pl.ds(pl.multiple_of(j * own_width, own_width), own_width)
        return pltpu.make_async_copy(wo_hbm.at[:, at], wo.at[j], wo_sem)

    core = own_place % 2
    spot = own_place // 2
    chip = me // 2
    partner = me + 1 - 2 * core
    lanes = 128
    chips = n_seq // 2
    chips_x = 2
    joined = requests - 2
    unforwarded = 1

    rows_y = requests // chips_x

    def request_at(i):
        y = own_request // chips_x
        row = (y, y + 1 - 2 * (y % 2), (y + 2) % rows_y, rows_y - 1 - y)[ORDER[i][0]]
        return row * chips_x + (own_request + ORDER[i][1]) % chips_x

    start_weights(wq_hbm, 0, 0, 0)

    barrier = pltpu.get_barrier_semaphore()

    def greet_seq(j, _):
        pl.semaphore_signal(
            barrier,
            inc=1,
            device_id=((me + j) % n_seq, head),
            device_id_type=pl.DeviceIdType.MESH,
        )
        return 0

    def greet_head(j, _):
        pl.semaphore_signal(
            barrier,
            inc=1,
            device_id=(me, (head + j) % n_head),
            device_id_type=pl.DeviceIdType.MESH,
        )
        return 0

    for n in sorted(range(1, n_head), key=lambda d: -min(d, n_head - d)):
        greet_head(n, 0)
    lax.fori_loop(1, n_seq, greet_seq, 0)

    for n in range(1, pieces):
        start_weights(wq_hbm, n * wide, n * wide, n)
    for copy in small[2:]:
        copy.start()

    def start_wo(j, _):
        wo_copy(j).start()
        return 0

    small[0].wait()
    small[1].wait()
    inputs = tokens_ref[...].astype(F32)
    mean = jnp.mean(inputs * inputs, axis=-1, keepdims=True)
    normed[...] = (
        inputs
        * lax.rsqrt(mean + NORM_EPSILON)
        * gain_ref[...].reshape(1, width).astype(F32)
    ).astype(BF16)

    for n in range(pieces):
        projected = project(n)
        if n == 0:
            start_weights(wk_hbm, 0, q_width, pieces)
            start_weights(wv_hbm, 0, q_width + HEAD_WIDTH, pieces)
        for g in range(2):
            line = (n * 2 + g) * rows
            qall[me, line : line + rows, :] = projected[
                :, g * HEAD_WIDTH : (g + 1) * HEAD_WIDTH
            ]

    def remote(source, target, send_sem, recv_sem, peer):
        return pltpu.make_async_remote_copy(
            src_ref=source,
            dst_ref=target,
            send_sem=send_sem,
            recv_sem=recv_sem,
            device_id=(peer, head),
            device_id_type=pl.DeviceIdType.MESH,
        )

    def arrived(ref, count, sem):
        at = pl.ds(0, count)
        pltpu.make_async_copy(ref.at[at], ref.at[at], sem).wait()

    def q_copy(which, recv_sem, peer):
        return remote(qall.at[which], qall.at[which], q_send_sem, recv_sem, peer)

    pl.semaphore_wait(barrier, n_seq - 1 + n_head - 1)

    def q_send(i):
        for n in range(2):
            to = request_at(i) * owners + (spot + n) % 2 * 2
            q_copy(me, q_far_sem.at[own_request], to + core).start()
            if i < unforwarded:
                q_copy(me, q_near_sem.at[own_request], to + 1 - core).start()

    q_send(0)
    q_send(1)
    for i in range(requests):
        r = request_at(i)
        for source, target in ((keys_hbm, keys), (values_hbm, values)):
            pltpu.make_async_copy(source.at[r], target.at[r], cache_sem.at[r]).start()
    lax.fori_loop(0, n_head, start_wo, 0)

    projected = project(pieces)
    for n in range(2):
        kvtree[own_place, n * rows : (n + 1) * rows, :] = projected[
            :, n * HEAD_WIDTH : (n + 1) * HEAD_WIDTH
        ]

    q_send(3)
    q_send(2)

    for copy in small[2:]:
        copy.wait()
    parent = parents_ref[pl.ds(own_request, 1), :]
    node = lax.broadcasted_iota(jnp.int32, (TREE, TREE), 0)
    other = lax.broadcasted_iota(jnp.int32, (TREE, TREE), 1)
    reached = jnp.where((parent == node) | (node == other), 1.0, 0.0)
    for _ in range(max(1, (TREE - 1).bit_length())):
        half = reached.astype(BF16)
        reached = jnp.minimum(jnp.dot(half, half, preferred_element_type=F32), 1.0)

    for n in range(1, owners):
        peer = own_request * owners + (own_place + n) % owners
        mine = kvtree.at[own_place]
        remote(mine, mine, kv_send_sem, kv_recv_sem, peer).start()
    q_send(4)
    q_send(5)

    row_in_page = lax.broadcasted_iota(jnp.int32, (PAGE, queries), 0)

    def forward(i):
        r = request_at(i)
        base = r * owners + core
        if i == requests - 1:
            arrived(qall, 1, q_far_sem.at[r])
            q_copy(beside, q_near_sem.at[r], partner).start()
        else:
            arrived(qall, 2, q_far_sem.at[r])
            q_copy(base, q_near_sem.at[r], partner).start()
            q_copy(base + 2, q_near_sem.at[r], partner).start()

    def wait_for(i):
        r = request_at(i)
        if i < unforwarded:
            arrived(qall, 2, q_far_sem.at[r])
        arrived(qall, 2, q_near_sem.at[r])
        arrived(keys, 2, cache_sem.at[r])

    def score_tile(i, b, best, score):
        r = request_at(i)
        q = qall[pl.ds(r * owners, owners)].reshape(queries, HEAD_WIDTH)
        s = lax.dot_general(
            keys[r, b * SCORE_TILE : (b + 1) * SCORE_TILE, :],
            q,
            NT,
            preferred_element_type=F32,
        )
        for n in range(SCORE_TILE // PAGE):
            p = b * (SCORE_TILE // PAGE) + n
            left = lengths_ref[r] - slots_ref[r, p] * PAGE
            shown = jnp.where(
                row_in_page < left, s[n * PAGE : (n + 1) * PAGE], HIDDEN
            )
            score[p * PAGE : (p + 1) * PAGE, :] = shown
            high = jnp.max(shown.reshape(PAGE // 8, 8, queries), axis=0)
            best = high if best is None else jnp.maximum(best, high)
        return best

    def weigh_tile(i, b, state, score, top):
        r = request_at(i)
        acc, total = state
        w = jnp.exp2(score[b * KEY_TILE : (b + 1) * KEY_TILE, :] * scale2 - top)
        low = jnp.sum(w.reshape(KEY_TILE // 8, 8, queries), axis=0)
        added = lax.dot_general(
            values[r, b * KEY_TILE : (b + 1) * KEY_TILE, :],
            w.astype(BF16),
            TN,
            preferred_element_type=F32,
        )
        if acc is None:
            return added, low
        return acc + added, total + low

    def finish(i, state, top, last):
        acc, total = state
        total = jnp.maximum(jnp.sum(total, axis=0, keepdims=True), 1.0)
        out = acc / total
        lse = top * (1.0 / math.log2(math.e)) + jnp.log(total)
        for n in range(2):
            half = slice(n * lanes, (n + 1) * lanes)
            lse_own[i, n] = lse[:, half]
            if not last:
                out_own[i, n] = out[:, half].astype(BF16)
        if last:
            out = out.T.astype(BF16).reshape(owners, block, HEAD_WIDTH)
            out_last[i - joined] = out

    def swap(i):
        other = 1 - core
        remote(
            out_own.at[i, other], out_swap.at[i], x_send_sem, x_recv_sem.at[i], partner
        ).start()
        remote(
            lse_own.at[i, other],
            lse_swap.at[i],
            xl_send_sem,
            xl_recv_sem.at[i],
            partner,
        ).start()

    def wait_swap(i):
        arrived(out_swap, 1, x_recv_sem.at[i])
        arrived(lse_swap, 1, xl_recv_sem.at[i])

    def join(i):
        mine, theirs = lse_own[i, core], lse_swap[i]
        high = jnp.maximum(mine, theirs)
        mine = jnp.exp(mine - high)
        theirs = jnp.exp(theirs - high)
        total = mine + theirs
        out = out_own[i, core].astype(F32) * (mine / total)
        out += out_swap[i].astype(F32) * (theirs / total)
        out_pair[i] = out.T.astype(BF16).reshape(2, block, HEAD_WIDTH)
        lse_pair[i] = high + jnp.log(total)

    def send_pair(i):
        first = request_at(i) * owners + core * 2

        for n in range(2):
            place = (core + n) % 2
            peer = first + place
            remote(
                out_pair.at[i, place], out_recv.at[chip], o_send_sem, o_recv_sem, peer
            ).start()
            remote(
                lse_pair.at[i], lse_recv.at[chip], l_send_sem, l_recv_sem, peer
            ).start()

    def send_direct(i):
        r = request_at(i)
        own = i == requests - 1
        spare = chips + (i - joined) * 2 + chip % 2
        slot = chip * (1 - core) + spare * core

        def send(n, _):
            place = (own_place + n) % owners
            peer = r * owners + place
            remote(
                out_last.at[i - joined, place],
                out_recv.at[slot],
                o_send_sem,
                o_recv_sem,
                peer,
            ).start()
            remote(
                lse_own.at[i, place // 2],
                lse_recv.at[slot],
                l_send_sem,
                l_recv_sem,
                peer,
            ).start()
            return 0

        lax.fori_loop(1 if own else 0, owners, send, 0)
        if own:
            out_recv[slot] = out_last[i - joined, own_place]
            lse_recv[slot] = lse_own[i, spot]

    def half_step(i, now, after):
        joins = 2 <= i < requests - 1
        direct = i >= joined
        for n in FORWARDS[i]:
            forward(n)
        if after is not None:
            wait_for(i + 1)
        if joins:
            wait_swap(i - 2)
        score, top_ref = now
        top = jnp.max(top_ref[...], axis=0, keepdims=True) * scale2
        state = (None, None)
        best = None
        for b in range(tiles):
            state = weigh_tile(i, b, state, score, top)
            if after is not None and b % every == 0:
                best = score_tile(i + 1, b // every, best, after[0])
        if after is not None:
            after[1][...] = best
        finish(i, state, top, direct)
        if joins:
            join(i - 2)
        if direct:
            send_direct(i)
        else:
            swap(i)
        if joins:
            send_pair(i - 2)
        if i == joined:
            wait_swap(i - 1)
            join(i - 1)
            send_pair(i - 1)

    a, b = (score_a, top_a), (score_b, top_b)
    wait_for(0)
    forward(1)
    best = None
    for t in range(tiles // every):
        best = score_tile(0, t, best, score_a)
    top_a[...] = best
    q_send(6)
    q_copy(me, q_near_sem.at[own_request], partner).start()
    beside = own_request * owners + (1 - spot) * 2 + core
    q_copy(me, q_far_sem.at[own_request], beside).start()
    for n in range(requests // 2):
        for i, now, after in ((2 * n, a, b), (2 * n + 1, b, a)):
            half_step(i, now, after if i < requests - 1 else None)

    arrived(kvtree, owners - 1, kv_recv_sem)
    own_queries = qall[me]
    own_queries = jnp.concatenate([own_queries] * (lanes // block), axis=0)
    tree_keys = kvtree[:, :rows, :].reshape(TREE, HEAD_WIDTH)
    tree_values = kvtree[:, rows:, :].reshape(TREE, HEAD_WIDTH)
    token = lax.broadcasted_iota(jnp.int32, (TREE, lanes), 0)
    lane = lax.broadcasted_iota(jnp.int32, (TREE, lanes), 1)
    pick = jnp.where(token == own_place * rows + lane % rows, 1.0, 0.0).astype(BF16)
    seen = jnp.dot(reached.astype(BF16), pick, preferred_element_type=F32) > 0.5
    tree_scores = lax.dot_general(
        tree_keys, own_queries, NT, preferred_element_type=F32
    )
    tree_scores = jnp.where(seen, tree_scores, HIDDEN)
    tree_top = jnp.max(tree_scores, axis=0, keepdims=True)
    tree_weights = jnp.where(
        seen, jnp.exp2(tree_scores * scale2 - tree_top * scale2), 0.0
    )
    tree_total = jnp.maximum(jnp.sum(tree_weights, axis=0, keepdims=True), 1.0)
    tree_sum = lax.dot_general(
        tree_values, tree_weights.astype(BF16), TN, preferred_element_type=F32
    )
    blocks = chips + 2 * (requests - joined)
    out_recv[blocks] = (tree_sum / tree_total).T[:block].astype(BF16)
    lse_recv[blocks] = tree_top * scale + jnp.log(tree_total)
    for n in range(blocks + 1, lse_recv.shape[0]):
        lse_recv[n] = jnp.full((1, lanes), HIDDEN, F32)
    arrived(wo, n_head, wo_sem)

    arrived(lse_recv, blocks - 1, l_recv_sem)
    lse = lse_recv[...].reshape(lse_recv.shape[0], lanes)
    lse = pltpu.roll(lse, (lanes - core * block) % lanes, 1)
    factor = jnp.exp(lse - jnp.max(lse, axis=0, keepdims=True))
    factor = (factor / jnp.sum(factor, axis=0, keepdims=True)).T[:block]
    arrived(out_recv, blocks - 1, o_recv_sem)
    merged = jnp.zeros((block, HEAD_WIDTH), F32)
    for n in range(blocks + 1):
        merged += out_recv[n].astype(F32) * factor[:, n : n + 1]
    merged = merged.astype(BF16)
    attended = jnp.concatenate(
        [merged[g * rows : (g + 1) * rows] for g in range(groups)], axis=1
    )

    def piece(j):
        return jnp.dot(attended, wo[j], preferred_element_type=F32)

    def part_copy(j):
        return pltpu.make_async_remote_copy(
            src_ref=part_send.at[j],
            dst_ref=part_recv.at[head],
            send_sem=p_send_sem,
            recv_sem=p_recv_sem,
            device_id=(me, j),
            device_id_type=pl.DeviceIdType.MESH,
        )

    order = sorted(range(1, n_head), key=lambda d: -min(d, n_head - d))
    for d in order:
        j = (head + d) % n_head
        part_send[j] = piece(j).astype(BF16)
        part_copy(j).start()
    mine = piece(head)
    at = pl.ds(pl.multiple_of(head * own_width, own_width), own_width)
    mine = mine + tokens_ref[:, at].astype(F32)
    part_recv[head] = jnp.zeros((rows, own_width), BF16)
    arrived(part_recv, n_head - 1, p_recv_sem)
    mixed_ref[...] = (mine + jnp.sum(part_recv[...].astype(F32), axis=0)).astype(BF16)

    arrived(part_send, n_head - 1, p_send_sem)
    arrived(qall, n_seq - 1, q_send_sem)
    arrived(kvtree, owners - 1, kv_send_sem)
    arrived(out_swap, joined, x_send_sem)
    arrived(lse_swap, joined, xl_send_sem)
    arrived(out_recv, blocks - 1, o_send_sem)
    arrived(lse_recv, blocks - 1, l_send_sem)


def per_device(
    tokens,
    norm_gain,
    w_query,
    key_projection,
    value_projection,
    w_out,
    cache_keys,
    paged_value_cache,
    lengths,
    parents,
    slot_block,
):
    n_seq = lax.axis_size("seq")
    n_head = lax.axis_size("head")
    rows, width = tokens.shape
    requests, context, _ = cache_keys.shape
    q_width = w_query.shape[1]
    groups = q_width // HEAD_WIDTH
    owners = TREE // rows
    block = groups * rows
    queries = owners * block
    own_width = width // n_head
    vmem = pl.BlockSpec(memory_space=pltpu.VMEM)
    hbm = pl.BlockSpec(memory_space=pltpu.HBM)
    dma = pltpu.SemaphoreType.DMA
    return pl.pallas_call(
        functools.partial(layer, n_seq, n_head),
        out_shape=pltpu.VMEM((rows, own_width), BF16),
        in_specs=[hbm] * 11,
        out_specs=vmem,
        scratch_shapes=[
            pltpu.SMEM(lengths.shape, jnp.int32),
            pltpu.SMEM(slot_block.shape, jnp.int32),
            pltpu.VMEM(tokens.shape, BF16),
            pltpu.VMEM(norm_gain.shape, BF16),
            pltpu.VMEM(parents.shape, jnp.int32),
            dma((5,)),
            pltpu.VMEM((width, q_width + 2 * HEAD_WIDTH), BF16),
            pltpu.VMEM((n_head, q_width, own_width), BF16),
            pltpu.VMEM((requests, context, HEAD_WIDTH), BF16),
            pltpu.VMEM((requests, context, HEAD_WIDTH), BF16),
            pltpu.VMEM((rows, width), BF16),
            pltpu.VMEM((n_seq, block, HEAD_WIDTH), BF16),
            pltpu.VMEM((owners, 2 * rows, HEAD_WIDTH), BF16),
            pltpu.VMEM((context, queries), F32),
            pltpu.VMEM((context, queries), F32),
            pltpu.VMEM((8, queries), F32),
            pltpu.VMEM((8, queries), F32),
            pltpu.VMEM((requests, 2, HEAD_WIDTH, 2 * block), BF16),
            pltpu.VMEM((requests, 2, 1, 2 * block), F32),
            pltpu.VMEM((requests, HEAD_WIDTH, 2 * block), BF16),
            pltpu.VMEM((requests, 1, 2 * block), F32),
            pltpu.VMEM((requests, 2, block, HEAD_WIDTH), BF16),
            pltpu.VMEM((requests, 1, 2 * block), F32),
            pltpu.VMEM((2, owners, block, HEAD_WIDTH), BF16),
            pltpu.VMEM((24, block, HEAD_WIDTH), BF16),
            pltpu.VMEM((24, 1, 2 * block), F32),
            pltpu.VMEM((n_head, rows, own_width), BF16),
            pltpu.VMEM((n_head, rows, own_width), BF16),
            dma((q_width // (2 * HEAD_WIDTH) + 1, 2)),
            dma,
            dma((requests,)),
            dma,
            dma((requests,)),
            dma((requests,)),
            dma,
            dma,
            dma,
            dma((requests - 2,)),
            dma,
            dma((requests - 2,)),
            dma,
            dma,
            dma,
            dma,
            dma,
            dma,
        ],
        compiler_params=pltpu.CompilerParams(
            collective_id=0,
            has_side_effects=True,
            vmem_limit_bytes=60 * 1024 * 1024,
        ),
        name="layer",
    )(
        lengths,
        slot_block,
        tokens,
        norm_gain,
        parents,
        w_query,
        key_projection,
        value_projection,
        w_out,
        cache_keys,
        paged_value_cache,
    )


def solution(mesh):
    in_specs = (
        P("seq", None),
        P(),
        P(None, "head"),
        P(None, "head"),
        P(None, "head"),
        P("head", None),
        P(None, "seq", "head"),
        P(None, "seq", "head"),
        P(),
        P(),
        P(None, "seq"),
    )
    return jax.shard_map(
        per_device,
        mesh=mesh,
        in_specs=in_specs,
        out_specs=P("seq", "head"),
        check_vma=False,
    )
```

```python
import functools
import math

import jax
import jax.numpy as jnp
from jax import lax
from jax.experimental import pallas as pl
from jax.experimental.pallas import tpu as pltpu
from jax.sharding import PartitionSpec as P

NORM_EPSILON = 1e-05
HIDDEN = -1e30
HEAD_WIDTH = 128
TREE = 64
PAGE = 128
KEY_TILE = 256
SCORE_TILE = 256
WEIGHT_PARTS = 4
ORDER = ((0, 1), (3, 0), (2, 0), (2, 1), (3, 1), (1, 1), (1, 0), (0, 0))
FORWARDS = ((2,), (3, 4), (5,), (6,), (7,), (), (), ())

NT = (((1,), (1,)), ((), ()))
TN = (((0,), (0,)), ((), ()))
F32 = jnp.float32
BF16 = jnp.bfloat16


def layer(
    n_seq,
    n_head,
    lengths_hbm,
    slots_hbm,
    tokens_hbm,
    gain_hbm,
    parents_hbm,
    wq_hbm,
    wk_hbm,
    wv_hbm,
    wo_hbm,
    keys_hbm,
    values_hbm,
    mixed_ref,
    lengths_ref,
    slots_ref,
    tokens_ref,
    gain_ref,
    parents_ref,
    small_sem,
    wqkv,
    wo,
    keys,
    values,
    normed,
    qall,
    kvtree,
    score_a,
    score_b,
    top_a,
    top_b,
    out_own,
    lse_own,
    out_swap,
    lse_swap,
    out_pair,
    lse_pair,
    out_last,
    out_recv,
    lse_recv,
    part_send,
    part_recv,
    w_sem,
    wo_sem,
    cache_sem,
    q_send_sem,
    q_far_sem,
    q_near_sem,
    kv_send_sem,
    kv_recv_sem,
    x_send_sem,
    x_recv_sem,
    xl_send_sem,
    xl_recv_sem,
    o_send_sem,
    o_recv_sem,
    l_send_sem,
    l_recv_sem,
    p_send_sem,
    p_recv_sem,
):
    me = lax.axis_index("seq")
    head = lax.axis_index("head")
    rows, width = tokens_ref.shape
    requests = keys.shape[0]
    context = keys.shape[1]
    owners = TREE // rows
    q_width = wq_hbm.shape[1]
    groups = q_width // HEAD_WIDTH
    block = groups * rows
    queries = owners * block
    tiles = context // KEY_TILE
    every = SCORE_TILE // KEY_TILE
    own_request = me // owners
    own_place = me % owners
    scale = HEAD_WIDTH**-0.5
    scale2 = scale * math.log2(math.e)

    small = [
        pltpu.make_async_copy(source, target, small_sem.at[n])
        for n, (source, target) in enumerate(
            (
                (tokens_hbm, tokens_ref),
                (gain_hbm, gain_ref),
                (parents_hbm, parents_ref),
                (lengths_hbm, lengths_ref),
                (slots_hbm, slots_ref),
            )
        )
    ]
    for copy in small[:2]:
        copy.start()
    part = width // WEIGHT_PARTS

    wide = 2 * HEAD_WIDTH
    pieces = q_width // wide

    halves = 2
    deep = width // halves

    def start_weights(source, first, column, sem):
        for c in range(WEIGHT_PARTS):
            at = pl.ds(c * part, part)
            count = min(wide, source.shape[1])
            pltpu.make_async_copy(
                source.at[at, pl.ds(first, count)],
                wqkv.at[at, pl.ds(column, count)],
                w_sem.at[sem, c * halves // WEIGHT_PARTS],
            ).start()

    def project(n):
        total = None
        for h in range(halves):
            at = wqkv.at[pl.ds(h * deep, deep), pl.ds(n * wide, wide)]
            pltpu.make_async_copy(at, at, w_sem.at[n, h]).wait()
            added = jnp.dot(
                normed[:, h * deep : (h + 1) * deep],
                wqkv[h * deep : (h + 1) * deep, n * wide : (n + 1) * wide],
                preferred_element_type=F32,
            )
            total = added if total is None else total + added
        return total.astype(BF16)

    own_width = width // n_head

    def wo_copy(j):
        at = pl.ds(pl.multiple_of(j * own_width, own_width), own_width)
        return pltpu.make_async_copy(wo_hbm.at[:, at], wo.at[j], wo_sem)

    core = own_place % 2
    spot = own_place // 2
    chip = me // 2
    partner = me + 1 - 2 * core
    lanes = 128
    chips = n_seq // 2
    chips_x = 2
    joined = requests - 2
    unforwarded = 1

    rows_y = requests // chips_x

    def request_at(i):
        y = own_request // chips_x
        row = (y, y + 1 - 2 * (y % 2), (y + 2) % rows_y, rows_y - 1 - y)[ORDER[i][0]]
        return row * chips_x + (own_request + ORDER[i][1]) % chips_x

    start_weights(wq_hbm, 0, 0, 0)

    barrier = pltpu.get_barrier_semaphore()

    def greet_seq(j, _):
        pl.semaphore_signal(
            barrier,
            inc=1,
            device_id=((me + j) % n_seq, head),
            device_id_type=pl.DeviceIdType.MESH,
        )
        return 0

    def greet_head(j, _):
        pl.semaphore_signal(
            barrier,
            inc=1,
            device_id=(me, (head + j) % n_head),
            device_id_type=pl.DeviceIdType.MESH,
        )
        return 0

    for n in sorted(range(1, n_head), key=lambda d: -min(d, n_head - d)):
        greet_head(n, 0)
    lax.fori_loop(1, n_seq, greet_seq, 0)

    for n in range(1, pieces):
        start_weights(wq_hbm, n * wide, n * wide, n)
    for copy in small[2:]:
        copy.start()

    def start_wo(j, _):
        wo_copy(j).start()
        return 0

    small[0].wait()
    small[1].wait()
    inputs = tokens_ref[...].astype(F32)
    mean = jnp.mean(inputs * inputs, axis=-1, keepdims=True)
    normed[...] = (
        inputs
        * lax.rsqrt(mean + NORM_EPSILON)
        * gain_ref[...].reshape(1, width).astype(F32)
    ).astype(BF16)

    for n in range(pieces):
        projected = project(n)
        if n == 0:
            start_weights(wk_hbm, 0, q_width, pieces)
            start_weights(wv_hbm, 0, q_width + HEAD_WIDTH, pieces)
        for g in range(2):
            line = (n * 2 + g) * rows
            qall[me, line : line + rows, :] = projected[
                :, g * HEAD_WIDTH : (g + 1) * HEAD_WIDTH
            ]

    def remote(source, target, send_sem, recv_sem, peer):
        return pltpu.make_async_remote_copy(
            src_ref=source,
            dst_ref=target,
            send_sem=send_sem,
            recv_sem=recv_sem,
            device_id=(peer, head),
            device_id_type=pl.DeviceIdType.MESH,
        )

    def arrived(ref, count, sem):
        at = pl.ds(0, count)
        pltpu.make_async_copy(ref.at[at], ref.at[at], sem).wait()

    def q_copy(which, recv_sem, peer):
        return remote(qall.at[which], qall.at[which], q_send_sem, recv_sem, peer)

    pl.semaphore_wait(barrier, n_seq - 1 + n_head - 1)

    def q_send(i):
        for n in range(2):
            to = request_at(i) * owners + (spot + n) % 2 * 2
            q_copy(me, q_far_sem.at[own_request], to + core).start()
            if i < unforwarded:
                q_copy(me, q_near_sem.at[own_request], to + 1 - core).start()

    q_send(0)
    q_send(1)
    for i in range(requests):
        r = request_at(i)
        for source, target in ((keys_hbm, keys), (values_hbm, values)):
            pltpu.make_async_copy(source.at[r], target.at[r], cache_sem.at[r]).start()
    lax.fori_loop(0, n_head, start_wo, 0)

    projected = project(pieces)
    for n in range(2):
        kvtree[own_place, n * rows : (n + 1) * rows, :] = projected[
            :, n * HEAD_WIDTH : (n + 1) * HEAD_WIDTH
        ]

    q_send(3)
    q_send(2)

    for copy in small[2:]:
        copy.wait()
    parent = parents_ref[pl.ds(own_request, 1), :]
    node = lax.broadcasted_iota(jnp.int32, (TREE, TREE), 0)
    other = lax.broadcasted_iota(jnp.int32, (TREE, TREE), 1)
    reached = jnp.where((parent == node) | (node == other), 1.0, 0.0)
    for _ in range(max(1, (TREE - 1).bit_length())):
        half = reached.astype(BF16)
        reached = jnp.minimum(jnp.dot(half, half, preferred_element_type=F32), 1.0)

    for n in range(1, owners):
        peer = own_request * owners + (own_place + n) % owners
        mine = kvtree.at[own_place]
        remote(mine, mine, kv_send_sem, kv_recv_sem, peer).start()
    q_send(4)
    q_send(5)

    row_in_page = lax.broadcasted_iota(jnp.int32, (PAGE, queries), 0)

    def forward(i):
        r = request_at(i)
        base = r * owners + core
        if i == requests - 1:
            arrived(qall, 1, q_far_sem.at[r])
            q_copy(beside, q_near_sem.at[r], partner).start()
        else:
            arrived(qall, 2, q_far_sem.at[r])
            q_copy(base, q_near_sem.at[r], partner).start()
            q_copy(base + 2, q_near_sem.at[r], partner).start()

    def wait_for(i):
        r = request_at(i)
        if i < unforwarded:
            arrived(qall, 2, q_far_sem.at[r])
        arrived(qall, 2, q_near_sem.at[r])
        arrived(keys, 2, cache_sem.at[r])

    def score_tile(i, b, best, score):
        r = request_at(i)
        q = qall[pl.ds(r * owners, owners)].reshape(queries, HEAD_WIDTH)
        s = lax.dot_general(
            keys[r, b * SCORE_TILE : (b + 1) * SCORE_TILE, :],
            q,
            NT,
            preferred_element_type=F32,
        )
        for n in range(SCORE_TILE // PAGE):
            p = b * (SCORE_TILE // PAGE) + n
            left = lengths_ref[r] - slots_ref[r, p] * PAGE
            shown = jnp.where(
                row_in_page < left, s[n * PAGE : (n + 1) * PAGE], HIDDEN
            )
            score[p * PAGE : (p + 1) * PAGE, :] = shown
            high = jnp.max(shown.reshape(PAGE // 8, 8, queries), axis=0)
            best = high if best is None else jnp.maximum(best, high)
        return best

    def weigh_tile(i, b, state, score, top):
        r = request_at(i)
        acc, total = state
        w = jnp.exp2(score[b * KEY_TILE : (b + 1) * KEY_TILE, :] * scale2 - top)
        low = jnp.sum(w.reshape(KEY_TILE // 8, 8, queries), axis=0)
        added = lax.dot_general(
            values[r, b * KEY_TILE : (b + 1) * KEY_TILE, :],
            w.astype(BF16),
            TN,
            preferred_element_type=F32,
        )
        if acc is None:
            return added, low
        return acc + added, total + low

    def finish(i, state, top, last):
        acc, total = state
        total = jnp.maximum(jnp.sum(total, axis=0, keepdims=True), 1.0)
        out = acc / total
        lse = top * (1.0 / math.log2(math.e)) + jnp.log(total)
        for n in range(2):
            half = slice(n * lanes, (n + 1) * lanes)
            lse_own[i, n] = lse[:, half]
            if not last:
                out_own[i, n] = out[:, half].astype(BF16)
        if last:
            out = out.T.astype(BF16).reshape(owners, block, HEAD_WIDTH)
            out_last[i - joined] = out

    def swap(i):
        other = 1 - core
        remote(
            out_own.at[i, other], out_swap.at[i], x_send_sem, x_recv_sem.at[i], partner
        ).start()
        remote(
            lse_own.at[i, other],
            lse_swap.at[i],
            xl_send_sem,
            xl_recv_sem.at[i],
            partner,
        ).start()

    def wait_swap(i):
        arrived(out_swap, 1, x_recv_sem.at[i])
        arrived(lse_swap, 1, xl_recv_sem.at[i])

    def join(i):
        mine, theirs = lse_own[i, core], lse_swap[i]
        high = jnp.maximum(mine, theirs)
        mine = jnp.exp(mine - high)
        theirs = jnp.exp(theirs - high)
        total = mine + theirs
        out = out_own[i, core].astype(F32) * (mine / total)
        out += out_swap[i].astype(F32) * (theirs / total)
        out_pair[i] = out.T.astype(BF16).reshape(2, block, HEAD_WIDTH)
        lse_pair[i] = high + jnp.log(total)

    def send_pair(i):
        first = request_at(i) * owners + core * 2

        for n in range(2):
            place = (core + n) % 2
            peer = first + place
            remote(
                out_pair.at[i, place], out_recv.at[chip], o_send_sem, o_recv_sem, peer
            ).start()
            remote(
                lse_pair.at[i], lse_recv.at[chip], l_send_sem, l_recv_sem, peer
            ).start()

    def send_direct(i):
        r = request_at(i)
        own = i == requests - 1
        spare = chips + (i - joined) * 2 + chip % 2
        slot = chip * (1 - core) + spare * core

        def send(n, _):
            place = (own_place + n) % owners
            peer = r * owners + place
            remote(
                out_last.at[i - joined, place],
                out_recv.at[slot],
                o_send_sem,
                o_recv_sem,
                peer,
            ).start()
            remote(
                lse_own.at[i, place // 2],
                lse_recv.at[slot],
                l_send_sem,
                l_recv_sem,
                peer,
            ).start()
            return 0

        lax.fori_loop(1 if own else 0, owners, send, 0)
        if own:
            out_recv[slot] = out_last[i - joined, own_place]
            lse_recv[slot] = lse_own[i, spot]

    def half_step(i, now, after):
        joins = 2 <= i < requests - 1
        direct = i >= joined
        for n in FORWARDS[i]:
            forward(n)
        if after is not None:
            wait_for(i + 1)
        if joins:
            wait_swap(i - 2)
        score, top_ref = now
        top = jnp.max(top_ref[...], axis=0, keepdims=True) * scale2
        state = (None, None)
        best = None
        for b in range(tiles):
            state = weigh_tile(i, b, state, score, top)
            if after is not None and b % every == 0:
                best = score_tile(i + 1, b // every, best, after[0])
        if after is not None:
            after[1][...] = best
        finish(i, state, top, direct)
        if joins:
            join(i - 2)
        if direct:
            send_direct(i)
        else:
            swap(i)
        if joins:
            send_pair(i - 2)
        if i == joined:
            wait_swap(i - 1)
            join(i - 1)
            send_pair(i - 1)

    a, b = (score_a, top_a), (score_b, top_b)
    wait_for(0)
    forward(1)
    best = None
    for t in range(tiles // every):
        best = score_tile(0, t, best, score_a)
    top_a[...] = best
    q_send(6)
    q_copy(me, q_near_sem.at[own_request], partner).start()
    beside = own_request * owners + (1 - spot) * 2 + core
    q_copy(me, q_far_sem.at[own_request], beside).start()
    for n in range(requests // 2):
        for i, now, after in ((2 * n, a, b), (2 * n + 1, b, a)):
            half_step(i, now, after if i < requests - 1 else None)

    arrived(kvtree, owners - 1, kv_recv_sem)
    own_queries = qall[me]
    own_queries = jnp.concatenate([own_queries] * (lanes // block), axis=0)
    tree_keys = kvtree[:, :rows, :].reshape(TREE, HEAD_WIDTH)
    tree_values = kvtree[:, rows:, :].reshape(TREE, HEAD_WIDTH)
    token = lax.broadcasted_iota(jnp.int32, (TREE, lanes), 0)
    lane = lax.broadcasted_iota(jnp.int32, (TREE, lanes), 1)
    pick = jnp.where(token == own_place * rows + lane % rows, 1.0, 0.0).astype(BF16)
    seen = jnp.dot(reached.astype(BF16), pick, preferred_element_type=F32) > 0.5
    tree_scores = lax.dot_general(
        tree_keys, own_queries, NT, preferred_element_type=F32
    )
    tree_scores = jnp.where(seen, tree_scores, HIDDEN)
    tree_top = jnp.max(tree_scores, axis=0, keepdims=True)
    tree_weights = jnp.where(
        seen, jnp.exp2(tree_scores * scale2 - tree_top * scale2), 0.0
    )
    tree_total = jnp.maximum(jnp.sum(tree_weights, axis=0, keepdims=True), 1.0)
    tree_sum = lax.dot_general(
        tree_values, tree_weights.astype(BF16), TN, preferred_element_type=F32
    )
    blocks = chips + 2 * (requests - joined)
    out_recv[blocks] = (tree_sum / tree_total).T[:block].astype(BF16)
    lse_recv[blocks] = tree_top * scale + jnp.log(tree_total)
    for n in range(blocks + 1, lse_recv.shape[0]):
        lse_recv[n] = jnp.full((1, lanes), HIDDEN, F32)
    arrived(wo, n_head, wo_sem)

    arrived(lse_recv, blocks - 1, l_recv_sem)
    lse = lse_recv[...].reshape(lse_recv.shape[0], lanes)
    lse = pltpu.roll(lse, (lanes - core * block) % lanes, 1)
    factor = jnp.exp(lse - jnp.max(lse, axis=0, keepdims=True))
    factor = (factor / jnp.sum(factor, axis=0, keepdims=True)).T[:block]
    arrived(out_recv, blocks - 1, o_recv_sem)
    merged = jnp.zeros((block, HEAD_WIDTH), F32)
    for n in range(blocks + 1):
        merged += out_recv[n].astype(F32) * factor[:, n : n + 1]
    merged = merged.astype(BF16)
    attended = jnp.concatenate(
        [merged[g * rows : (g + 1) * rows] for g in range(groups)], axis=1
    )

    def piece(j):
        return jnp.dot(attended, wo[j], preferred_element_type=F32)

    def part_copy(j):
        return pltpu.make_async_remote_copy(
            src_ref=part_send.at[j],
            dst_ref=part_recv.at[head],
            send_sem=p_send_sem,
            recv_sem=p_recv_sem,
            device_id=(me, j),
            device_id_type=pl.DeviceIdType.MESH,
        )

    order = sorted(range(1, n_head), key=lambda d: -min(d, n_head - d))
    for d in order:
        j = (head + d) % n_head
        part_send[j] = piece(j).astype(BF16)
        part_copy(j).start()
    mine = piece(head)
    at = pl.ds(pl.multiple_of(head * own_width, own_width), own_width)
    mine = mine + tokens_ref[:, at].astype(F32)
    part_recv[head] = jnp.zeros((rows, own_width), BF16)
    arrived(part_recv, n_head - 1, p_recv_sem)
    mixed_ref[...] = (mine + jnp.sum(part_recv[...].astype(F32), axis=0)).astype(BF16)

    arrived(part_send, n_head - 1, p_send_sem)
    arrived(qall, n_seq - 1, q_send_sem)
    arrived(kvtree, owners - 1, kv_send_sem)
    arrived(out_swap, joined, x_send_sem)
    arrived(lse_swap, joined, xl_send_sem)
    arrived(out_recv, blocks - 1, o_send_sem)
    arrived(lse_recv, blocks - 1, l_send_sem)


def per_device(
    tokens,
    norm_gain,
    w_query,
    key_projection,
    value_projection,
    w_out,
    cache_keys,
    paged_value_cache,
    lengths,
    parents,
    slot_block,
):
    n_seq = lax.axis_size("seq")
    n_head = lax.axis_size("head")
    rows, width = tokens.shape
    requests, context, _ = cache_keys.shape
    q_width = w_query.shape[1]
    groups = q_width // HEAD_WIDTH
    owners = TREE // rows
    block = groups * rows
    queries = owners * block
    own_width = width // n_head
    vmem = pl.BlockSpec(memory_space=pltpu.VMEM)
    hbm = pl.BlockSpec(memory_space=pltpu.HBM)
    dma = pltpu.SemaphoreType.DMA
    return pl.pallas_call(
        functools.partial(layer, n_seq, n_head),
        out_shape=pltpu.VMEM((rows, own_width), BF16),
        in_specs=[hbm] * 11,
        out_specs=vmem,
        scratch_shapes=[
            pltpu.SMEM(lengths.shape, jnp.int32),
            pltpu.SMEM(slot_block.shape, jnp.int32),
            pltpu.VMEM(tokens.shape, BF16),
            pltpu.VMEM(norm_gain.shape, BF16),
            pltpu.VMEM(parents.shape, jnp.int32),
            dma((5,)),
            pltpu.VMEM((width, q_width + 2 * HEAD_WIDTH), BF16),
            pltpu.VMEM((n_head, q_width, own_width), BF16),
            pltpu.VMEM((requests, context, HEAD_WIDTH), BF16),
            pltpu.VMEM((requests, context, HEAD_WIDTH), BF16),
            pltpu.VMEM((rows, width), BF16),
            pltpu.VMEM((n_seq, block, HEAD_WIDTH), BF16),
            pltpu.VMEM((owners, 2 * rows, HEAD_WIDTH), BF16),
            pltpu.VMEM((context, queries), F32),
            pltpu.VMEM((context, queries), F32),
            pltpu.VMEM((8, queries), F32),
            pltpu.VMEM((8, queries), F32),
            pltpu.VMEM((requests, 2, HEAD_WIDTH, 2 * block), BF16),
            pltpu.VMEM((requests, 2, 1, 2 * block), F32),
            pltpu.VMEM((requests, HEAD_WIDTH, 2 * block), BF16),
            pltpu.VMEM((requests, 1, 2 * block), F32),
            pltpu.VMEM((requests, 2, block, HEAD_WIDTH), BF16),
            pltpu.VMEM((requests, 1, 2 * block), F32),
            pltpu.VMEM((2, owners, block, HEAD_WIDTH), BF16),
            pltpu.VMEM((24, block, HEAD_WIDTH), BF16),
            pltpu.VMEM((24, 1, 2 * block), F32),
            pltpu.VMEM((n_head, rows, own_width), BF16),
            pltpu.VMEM((n_head, rows, own_width), BF16),
            dma((q_width // (2 * HEAD_WIDTH) + 1, 2)),
            dma,
            dma((requests,)),
            dma,
            dma((requests,)),
            dma((requests,)),
            dma,
            dma,
            dma,
            dma((requests - 2,)),
            dma,
            dma((requests - 2,)),
            dma,
            dma,
            dma,
            dma,
            dma,
            dma,
        ],
        compiler_params=pltpu.CompilerParams(
            collective_id=0,
            has_side_effects=True,
            vmem_limit_bytes=60 * 1024 * 1024,
        ),
        name="layer",
    )(
        lengths,
        slot_block,
        tokens,
        norm_gain,
        parents,
        w_query,
        key_projection,
        value_projection,
        w_out,
        cache_keys,
        paged_value_cache,
    )


def solution(mesh):
    in_specs = (
        P("seq", None),
        P(),
        P(None, "head"),
        P(None, "head"),
        P(None, "head"),
        P("head", None),
        P(None, "seq", "head"),
        P(None, "seq", "head"),
        P(),
        P(),
        P(None, "seq"),
    )
    return jax.shard_map(
        per_device,
        mesh=mesh,
        in_specs=in_specs,
        out_specs=P("seq", "head"),
        check_vma=False,
    )
```
